16 devices in a mesh: tp: 4 (over z, y), ep: 4 (over x, core).
Axes of the slice: x: 2, y: 2, z: 2, core: 2. Of those that a mesh axis runs over, the one named last changes fastest.
Arguments:
- x: bfloat16 [1024, 1536], P(('ep', 'tp'))
- grad_y: bfloat16 [1024, 1536], P(('ep', 'tp'))
- w_router: bfloat16 [1536, 64], replicated
- w_gate: bfloat16 [64, 1536, 512], P('ep', None, 'tp')
- w_up: bfloat16 [64, 1536, 512], P('ep', None, 'tp')
- w_down: bfloat16 [64, 512, 1536], P('ep', 'tp')
- ws_gate: bfloat16 [1536, 1024], P(None, 'tp')
- ws_up: bfloat16 [1536, 1024], P(None, 'tp')
- ws_down: bfloat16 [1024, 1536], P('tp')
- topk_idx: int32 [1024, 6], P(('ep', 'tp'))
Outputs:
- output 1: bfloat16 [1024, 1536], P(('ep', 'tp'))
- output 2: bfloat16 [1024, 1536], P(('ep', 'tp'))
- output 3: float32 [1536, 64], replicated
- output 4: float32 [64, 1536, 512], P('ep', None, 'tp')
- output 5: float32 [64, 1536, 512], P('ep', None, 'tp')
- output 6: float32 [64, 512, 1536], P('ep', 'tp')
- output 7: float32 [1536, 1024], P(None, 'tp')
- output 8: float32 [1536, 1024], P(None, 'tp')
- output 9: float32 [1024, 1536], P('tp')
All inputs are finite; a program needn't handle non-finite values.
Results may differ from the reference program's by a relative error of at most 0.0143696.
Values are sent between devices in bfloat16 or wider.
A program may use at most 1 GiB of HBM per device.

```python
import jax
import jax.numpy as jnp
from jax import lax

D = 1536
EXPERTS = 64
FF = 512
SHARED_FF = 1024
TOP = 6
TOK = 64
TP = 4
EP = 4

GATE_SCALE = 16.0


def capacity():
    groups = TOP // 2
    most = groups * TOK // (2 * EP) + min(groups, EP // 2) * TOK // EP
    per_group = EXPERTS // EP
    return (2 * most + per_group - 1) // per_group


def draw_routes(key):
    devices = TP * EP
    groups = TOP // 2
    half_tok = TOK // 2
    per_group = EXPERTS // EP
    role_key, group_key, local_key = jax.random.split(key, 3)
    role_ids = jax.vmap(lambda sub_key: jax.random.permutation(sub_key, TOK))(jax.random.split(role_key, devices))
    base_group = jnp.where(role_ids < half_tok, role_ids % EP, role_ids % (EP // 2))
    visited = (base_group[:, :, None] + jnp.arange(groups)[None, None, :]) % EP
    hit_map = jax.nn.one_hot(visited.reshape(devices, TOK * groups), EP, dtype=jnp.int32)
    visit_num = jnp.sum((jnp.cumsum(hit_map, axis=1) - hit_map) * hit_map, axis=2).reshape(devices, TOK, groups)
    local_ids = (2 * visit_num[:, :, :, None] + jnp.arange(2)[None, None, None, :]) % per_group
    group_perm = jax.vmap(lambda sub_key: jax.random.permutation(sub_key, EP))(jax.random.split(group_key, devices))
    local_perm = jax.vmap(lambda sub_key: jax.random.permutation(sub_key, per_group))(jax.random.split(local_key, devices * EP)).reshape(devices, EP * per_group)
    true_group = jnp.take_along_axis(group_perm, visited.reshape(devices, TOK * groups), axis=1).reshape(devices, TOK, groups, 1)
    position = (true_group * per_group + local_ids).reshape(devices, TOK * TOP)
    local_pick = jnp.take_along_axis(local_perm, position, axis=1).reshape(devices, TOK, groups, 2)
    expert_ids = true_group * per_group + local_pick
    return expert_ids.reshape(devices * TOK, TOP).astype(jnp.int32)


def normal_bf16(key, arr_shape, std_dev):
    return (jax.random.normal(key, arr_shape, jnp.float32) * std_dev).astype(jnp.bfloat16)


def setup_inputs(seed: int = 0) -> dict:
    key_list = jax.random.split(jax.random.key(seed), 10)
    tokens = TOK * TP * EP
    return dict(
        x=normal_bf16(key_list[0], (tokens, D), 1.0),
        grad_y=normal_bf16(key_list[1], (tokens, D), 1.0),
        w_router=normal_bf16(key_list[2], (D, EXPERTS), D ** -0.5),
        w_gate=normal_bf16(key_list[3], (EXPERTS, D, FF), D ** -0.5),
        w_up=normal_bf16(key_list[4], (EXPERTS, D, FF), D ** -0.5),
        w_down=normal_bf16(key_list[5], (EXPERTS, FF, D), FF ** -0.5),
        ws_gate=normal_bf16(key_list[6], (D, SHARED_FF), D ** -0.5),
        ws_up=normal_bf16(key_list[7], (D, SHARED_FF), D ** -0.5),
        ws_down=normal_bf16(key_list[8], (SHARED_FF, D), SHARED_FF ** -0.5),
        topk_idx=draw_routes(key_list[9]),
    )


def swiglu(rows_in, w_a, w_b, w_c):
    gate_pre = jnp.dot(rows_in, w_a).astype(jnp.bfloat16).astype(jnp.float32)
    up_pre = jnp.dot(rows_in, w_b).astype(jnp.bfloat16).astype(jnp.float32)
    hidden = (jax.nn.silu(gate_pre) * up_pre).astype(jnp.bfloat16).astype(jnp.float32)
    return jnp.dot(hidden, w_c)


def reference(x, grad_y, w_router, w_gate, w_up, w_down, ws_gate, ws_up, ws_down, topk_idx):
    tokens = x.shape[0]
    cap_all = capacity() * TP * EP
    hit_count = jnp.sum(jax.nn.one_hot(topk_idx, EXPERTS, dtype=jnp.int32), axis=1)
    slot_rank = jnp.cumsum(hit_count, axis=0) - hit_count
    slot_of = topk_idx * cap_all + jnp.take_along_axis(slot_rank, topk_idx, axis=1)
    token_ids = jnp.broadcast_to(jnp.arange(tokens, dtype=jnp.int32)[:, None], slot_of.shape)
    slot_owner = jnp.zeros((EXPERTS * cap_all,), jnp.int32).at[slot_of.reshape(-1)].set(token_ids.reshape(-1)).reshape(EXPERTS, cap_all)

    def forward(x_wide, router_w, gate_w, up_w, down_w, sgate_w, sup_w, sdown_w):
        router_probs = jax.nn.softmax(jnp.dot(x_wide, router_w), axis=-1)
        route_gates = GATE_SCALE * jnp.take_along_axis(router_probs, topk_idx, axis=1)
        total = swiglu(x_wide, sgate_w, sup_w, sdown_w)

        def one_expert(operands):
            owner_ids, w_a, w_b, w_c = operands
            expert_rows = jnp.take(x_wide, owner_ids, axis=0).astype(jnp.bfloat16).astype(jnp.float32)
            return swiglu(expert_rows, w_a, w_b, w_c).astype(jnp.bfloat16)

        expert_out = lax.map(jax.checkpoint(one_expert), (slot_owner, gate_w, up_w, down_w)).reshape(EXPERTS * cap_all, D)
        for k in range(TOP):
            total = total + route_gates[:, k:k + 1] * jnp.take(expert_out, slot_of[:, k], axis=0).astype(jnp.float32)
        return total.astype(jnp.bfloat16)

    y_out, pullback = jax.vjp(forward, x.astype(jnp.float32), w_router.astype(jnp.float32), w_gate.astype(jnp.float32), w_up.astype(jnp.float32), w_down.astype(jnp.float32), ws_gate.astype(jnp.float32), ws_up.astype(jnp.float32), ws_down.astype(jnp.float32))
    grads = pullback(grad_y)
    return (y_out, grads[0].astype(jnp.bfloat16), grads[1], grads[2], grads[3], grads[4], grads[5], grads[6], grads[7])
```

```python
import functools

import jax
import jax.numpy as jnp
from jax import lax
from jax.experimental import pallas as pl
from jax.experimental.pallas import tpu as pltpu
from jax.sharding import PartitionSpec as P

GATE_SCALE = 16.0
BF = jnp.bfloat16
F32 = jnp.float32
MESH = pl.DeviceIdType.MESH

D = 1536
EXPERTS = 64
TOP = 6
TOK = 64
TP = 4
EP = 4
NDEV = TP * EP
LOCAL = EXPERTS // EP
CAP = 7
STRIP = 8
ROWS = NDEV * STRIP
PAIR_ROWS = 2 * EP * CAP
STEPS = LOCAL // 2
SH_ROWS = 2 * TOK // STEPS
BLK = PAIR_ROWS + SH_ROWS

BIT_Y, BIT_Z, BIT_C, BIT_X = 1, 2, 4, 8


def flip(value, bit):
    return value + bit * (1 - 2 * ((value // bit) % 2))


def flip_mask(value, mask):
    for bit in (1, 2, 4, 8):
        if mask & bit:
            value = flip(value, bit)
    return value


def dot(a, b):
    return jnp.dot(a, b, preferred_element_type=F32)


def dot_nt(a, b):
    return lax.dot_general(a, b, (((1,), (1,)), ((), ())), preferred_element_type=F32)


def dot_tn(a, b):
    return lax.dot_general(a, b, (((0,), (0,)), ((), ())), preferred_element_type=F32)


def act_both(a, b, dh):
    sig = 1.0 / (1.0 + jnp.exp(-a))
    silu = a * sig
    h = (silu * b).astype(BF)
    db = (dh * silu).astype(BF)
    da = (dh * b * (sig * (1.0 + a * (1.0 - sig)))).astype(BF)
    return h, da, db


def gather_kernel(rows_ref, tab_ref, all_ref, tabs_ref, send_sem, recv_sem, local_sem):
    tp = lax.axis_index('tp')
    ep = lax.axis_index('ep')
    me = ep * TP + tp
    third = D // 3

    def peer(mask):
        return (flip_mask(tp, mask & 3), flip_mask(ep, mask >> 2))

    barrier = pltpu.get_barrier_semaphore()
    for mask in (BIT_X, BIT_Y, BIT_Z, BIT_C):
        pl.semaphore_signal(barrier, inc=1, device_id=peer(mask), device_id_type=MESH)
    pl.semaphore_wait(barrier, 4)

    orders = [(BIT_X, BIT_Y, BIT_Z), (BIT_Y, BIT_Z, BIT_X), (BIT_Z, BIT_X, BIT_Y), (BIT_X, BIT_Y, BIT_Z)]

    def view(part, block, own):
        if part == 3:
            return tab_ref if own else tabs_ref.at[block]
        cols = pl.ds(part * third, third)
        return rows_ref.at[:, cols] if own else all_ref.at[block, :, cols]

    def copy(part, k, mask):
        block = flip_mask(me, k)
        return pltpu.make_async_remote_copy(
            src_ref=view(part, block, k == 0), dst_ref=view(part, block, False),
            send_sem=send_sem.at[part, k ^ mask], recv_sem=recv_sem.at[part, k ^ mask],
            device_id=peer(mask), device_id_type=MESH)

    sent = []

    def send(part, k, mask):
        c = copy(part, k, mask)
        c.start()
        sent.append(c)

    def arrived(part, k):
        block = flip_mask(me, k)
        pltpu.make_async_remote_copy(
            src_ref=view(part, block, False), dst_ref=view(part, block, False),
            send_sem=send_sem.at[part, k], recv_sem=recv_sem.at[part, k],
            device_id=peer(BIT_C), device_id_type=MESH).wait_recv()

    parts = (3, 0, 1, 2)
    for step in range(3):
        for part in parts:
            send(part, 0, orders[part][step])
    for part in parts:
        send(part, 0, BIT_C)
    own_rows = pltpu.make_async_copy(rows_ref, all_ref.at[me], local_sem.at[0])
    own_tab = pltpu.make_async_copy(tab_ref, tabs_ref.at[me], local_sem.at[1])
    own_rows.start()
    own_tab.start()
    for part in parts:
        m1, m2, m3 = orders[part]
        arrived(part, m1)
        send(part, m1, m2)
        send(part, m1, m3)
        send(part, m1, BIT_C)
    for part in parts:
        m1, m2, m3 = orders[part]
        arrived(part, m2)
        send(part, m2, m3)
        send(part, m2, BIT_C)
    for part in parts:
        m1, m2, m3 = orders[part]
        arrived(part, m1 ^ m2)
        send(part, m1 ^ m2, m3)
        send(part, m1 ^ m2, BIT_C)
    for extra in range(4):
        for part in parts:
            m1, m2, m3 = orders[part]
            k = (m3, m1 ^ m3, m2 ^ m3, m1 ^ m2 ^ m3)[extra]
            arrived(part, k)
            send(part, k, BIT_C)
    for part in parts:
        for k in range(16):
            if k & BIT_C:
                arrived(part, k)
    own_rows.wait()
    own_tab.wait()
    for c in sent:
        c.wait_send()


def gather_rows(rows, tab):
    vmem = pl.BlockSpec(memory_space=pltpu.VMEM)
    return pl.pallas_call(
        gather_kernel,
        name='gather_rows',
        out_shape=(jax.ShapeDtypeStruct((NDEV,) + rows.shape, rows.dtype), jax.ShapeDtypeStruct((NDEV,) + tab.shape, tab.dtype)),
        in_specs=[vmem, vmem],
        out_specs=(vmem, vmem),
        scratch_shapes=[pltpu.SemaphoreType.DMA((4, 16)), pltpu.SemaphoreType.DMA((4, 16)), pltpu.SemaphoreType.DMA((2,))],
        compiler_params=pltpu.CompilerParams(collective_id=0, has_side_effects=True, vmem_limit_bytes=40 << 20),
        cost_estimate=pl.CostEstimate(flops=40_000_000_000, bytes_accessed=7_000_000, transcendentals=0),
    )(rows, tab)


def main_kernel(g_ref, all_ref, slot_ref, wr_ref, wsg_ref, wsu_ref, wsd_ref, perm_ref, wg_ref, wu_ref, wd_ref,
                part_ref, h_ref, dab_ref, xe_hbm, de_hbm, xe, de, sh, sems):
    step = pl.program_id(0)
    g = g_ref[0]
    third = D // 3
    xe_copy = pltpu.make_async_copy(xe, xe_hbm, sems.at[0])
    de_copy = pltpu.make_async_copy(de, de_hbm, sems.at[1])

    @pl.when(step == 0)
    def _():
        n_rows = LOCAL * EP * STRIP
        lane = lax.broadcasted_iota(jnp.int32, (n_rows, EP * TOK), 1)
        wr = wr_ref[...]
        row_expert = g * LOCAL + lax.broadcasted_iota(jnp.int32, (n_rows, 3 * EXPERTS), 0) // (EP * STRIP)
        wanted = lax.broadcasted_iota(jnp.int32, (n_rows, 3 * EXPERTS), 1) % EXPERTS == row_expert
        for j in range(TP):
            pick = jnp.where(slot_ref[j] == lane, 1.0, 0.0).astype(BF)
            x_j = jnp.concatenate([all_ref[s * TP + j, :TOK, :] for s in range(EP)], axis=0)
            logits = dot(x_j, wr)
            top = jnp.max(logits, axis=-1, keepdims=True)
            ex = jnp.exp(logits - top)
            probs = ex / jnp.sum(ex, axis=-1, keepdims=True)
            hi = probs.astype(BF)
            rest = probs - hi.astype(F32)
            mid = rest.astype(BF)
            low = (rest - mid.astype(F32)).astype(BF)
            sel = dot(pick, jnp.concatenate([hi, mid, low], axis=1))
            gate = GATE_SCALE * jnp.sum(jnp.where(wanted, sel, 0.0), axis=1, keepdims=True)
            for n in range(3):
                cols = slice(n * third, (n + 1) * third)
                got = dot(pick, x_j[:, cols]).astype(BF)
                xe[:, EP * STRIP * j:EP * STRIP * (j + 1), cols] = got.reshape(LOCAL, EP * STRIP, third)
                gy_j = jnp.concatenate([all_ref[s * TP + j, TOK:, cols] for s in range(EP)], axis=0)
                got = (dot(pick, gy_j) * gate).astype(BF)
                de[:, EP * STRIP * j:EP * STRIP * (j + 1), cols] = got.reshape(LOCAL, EP * STRIP, third)
        xe_copy.start()
        de_copy.start()
        x_s = jnp.concatenate([all_ref[g * TP + j, :TOK, :] for j in range(TP)], axis=0)
        gy_s = jnp.concatenate([all_ref[g * TP + j, TOK:, :] for j in range(TP)], axis=0)
        a = dot(x_s, wsg_ref[...]).astype(BF).astype(F32)
        b = dot(x_s, wsu_ref[...]).astype(BF).astype(F32)
        dh = dot_nt(gy_s, wsd_ref[...]).astype(BF).astype(F32)
        h, da, db = act_both(a, b, dh)
        for n in range(3):
            cols = slice(n * third, (n + 1) * third)
            sh[0, :, :, cols] = dot(h, wsd_ref[:, cols]).reshape(TP, TOK, third)
            dxs = dot_nt(da, wsg_ref[cols, :]) + dot_nt(db, wsu_ref[cols, :])
            sh[1, :, :, cols] = dxs.reshape(TP, TOK, third)

    lhs = []
    for i in range(2):
        e = 2 * step + i
        x_e = xe[e]
        ab = dot(x_e, jnp.concatenate([wg_ref[i], wu_ref[i]], axis=1)).astype(BF).astype(F32)
        dh = dot_nt(de[e], wd_ref[i]).astype(BF).astype(F32)
        width = ab.shape[1] // 2
        h, da, db = act_both(ab[:, :width], ab[:, width:], dh)
        h_ref[i] = h
        dab = jnp.concatenate([da, db], axis=1)
        dab_ref[i] = dab
        lhs.append(dot(perm_ref[i], dab).astype(BF))
    lhs = jnp.concatenate(lhs, axis=1)
    for n in range(3):
        cols = slice(n * third, (n + 1) * third)
        rhs = jnp.concatenate([wg_ref[0, cols, :], wu_ref[0, cols, :], wg_ref[1, cols, :], wu_ref[1, cols, :]], axis=1)
        part_ref[:, :PAIR_ROWS, cols] = dot_nt(lhs, rhs).reshape(TP, PAIR_ROWS, third)
    half = step // (STEPS // 2)
    first = pl.multiple_of((step % (STEPS // 2)) * SH_ROWS, SH_ROWS)
    part_ref[:, PAIR_ROWS:, :] = sh[half, :, pl.ds(first, SH_ROWS), :]

    @pl.when(step == STEPS - 1)
    def _():
        xe_copy.wait()
        de_copy.wait()


def main_call(g, all_rows, slots, w_router, ws_gate, ws_up, ws_down, perm, w_gate, w_up, w_down):
    width = w_gate.shape[2]

    def whole(a):
        return pl.BlockSpec(a.shape, lambda i, g_: (0,) * a.ndim, pipeline_mode=pl.Buffered(1))

    def pair(a):
        return pl.BlockSpec((2,) + a.shape[1:], lambda i, g_: (i, 0, 0))

    any_spec = pl.BlockSpec(memory_space=pl.ANY)
    return pl.pallas_call(
        main_kernel,
        name='main_call',
        grid_spec=pltpu.PrefetchScalarGridSpec(
            num_scalar_prefetch=1,
            grid=(STEPS,),
            in_specs=[whole(all_rows), whole(slots), whole(w_router), whole(ws_gate), whole(ws_up), whole(ws_down), whole(perm),
                      pair(w_gate), pair(w_up), pair(w_down)],
            out_specs=[pl.BlockSpec((TP, BLK, D), lambda i, g_: (0, i, 0)),
                       pl.BlockSpec((2, ROWS, width), lambda i, g_: (i, 0, 0)),
                       pl.BlockSpec((2, ROWS, 2 * width), lambda i, g_: (i, 0, 0)), any_spec, any_spec],
            scratch_shapes=[pltpu.VMEM((LOCAL, ROWS, D), BF), pltpu.VMEM((LOCAL, ROWS, D), BF),
                            pltpu.VMEM((2, TP, TOK, D), F32), pltpu.SemaphoreType.DMA((2,))],
        ),
        out_shape=[jax.ShapeDtypeStruct((TP, BLK * STEPS, D), F32), jax.ShapeDtypeStruct((LOCAL, ROWS, width), BF),
                   jax.ShapeDtypeStruct((LOCAL, ROWS, 2 * width), BF),
                   jax.ShapeDtypeStruct((LOCAL, ROWS, D), BF), jax.ShapeDtypeStruct((LOCAL, ROWS, D), BF)],
        compiler_params=pltpu.CompilerParams(vmem_limit_bytes=58 << 20),
        cost_estimate=pl.CostEstimate(flops=20_000_000_000, bytes_accessed=60_000_000, transcendentals=4_000_000),
    )(g, all_rows, slots, w_router, ws_gate, ws_up, ws_down, perm, w_gate, w_up, w_down)


def grad_kernel(xe_ref, de_ref, h_ref, dab_ref, dg_ref, du_ref, dd_ref):
    both = dot_tn(xe_ref[0], dab_ref[0])
    width = both.shape[1] // 2
    dg_ref[0] = both[:, :width]
    du_ref[0] = both[:, width:]
    dd_ref[0] = dot_tn(h_ref[0], de_ref[0])


def grad_call(xe, de, h, dab):
    width = h.shape[2]

    def one(shape):
        return pl.BlockSpec((1,) + shape, lambda i: (i, 0, 0))

    return pl.pallas_call(
        grad_kernel,
        name='grad_call',
        grid=(LOCAL,),
        in_specs=[one((ROWS, D)), one((ROWS, D)), one((ROWS, width)), one((ROWS, 2 * width))],
        out_specs=[one((D, width)), one((D, width)), one((width, D))],
        out_shape=[jax.ShapeDtypeStruct((LOCAL, D, width), F32), jax.ShapeDtypeStruct((LOCAL, D, width), F32),
                   jax.ShapeDtypeStruct((LOCAL, width, D), F32)],
        compiler_params=pltpu.CompilerParams(vmem_limit_bytes=40 << 20),
        cost_estimate=pl.CostEstimate(flops=10_000_000_000, bytes_accessed=55_000_000, transcendentals=0),
    )(xe, de, h, dab)


def out_kernel(tp_ref, h0, h1, h2, h3, w0, w1, w2, w3, o_ref):
    total = dot(jnp.concatenate([h0[0], h1[0], h2[0], h3[0]], axis=1), jnp.concatenate([w0[0], w1[0], w2[0], w3[0]], axis=0))
    for j in range(TP):
        for s in range(EP):
            first = STRIP * (j * EP + s)
            o_ref[s * TP + j, 0] = total[first:first + STRIP].astype(BF)


def out_call(tp, h_own, h_in, w_own, w_in):
    width = h_own.shape[2]
    per = LOCAL // TP

    def own(shape):
        return pl.BlockSpec((1,) + shape, lambda i, t: (t[0] * per + i, 0, 0))

    def got(shape):
        return pl.BlockSpec((1,) + shape, lambda i, t: (i, 0, 0))

    return pl.pallas_call(
        out_kernel,
        name='out_call',
        grid_spec=pltpu.PrefetchScalarGridSpec(
            num_scalar_prefetch=1,
            grid=(per,),
            in_specs=[own((ROWS, width))] + [got((ROWS, width))] * 3 + [own((width, D))] + [got((width, D))] * 3,
            out_specs=pl.BlockSpec((NDEV, 1, STRIP, D), lambda i, t: (0, i, 0, 0)),
        ),
        out_shape=jax.ShapeDtypeStruct((NDEV, per, STRIP, D), BF),
        compiler_params=pltpu.CompilerParams(vmem_limit_bytes=40 << 20),
        cost_estimate=pl.CostEstimate(flops=5_000_000_000, bytes_accessed=10_000_000, transcendentals=0),
    )(tp, h_own, *h_in, w_own, *w_in)


def permutations():
    row = jnp.arange(TP * PAIR_ROWS)
    col, rest = row // PAIR_ROWS, row % PAIR_ROWS
    src, rest = rest // (2 * CAP), rest % (2 * CAP)
    which, slot = rest // CAP, rest % CAP
    wanted = col * (EP * STRIP) + src * STRIP + slot
    hit = wanted[:, None] == jnp.arange(ROWS)[None, :]
    return jnp.stack([hit & (which == i)[:, None] for i in range(2)]).astype(BF)


def solution(mesh):
    def device_step(x, grad_y, w_router, w_gate, w_up, w_down, ws_gate, ws_up, ws_down, topk_idx):
        tp = lax.axis_index('tp')
        ep = lax.axis_index('ep')
        per = LOCAL // TP
        w_down_in = []
        for m in range(1, TP):
            away = lax.dynamic_slice_in_dim(w_down, (tp ^ m) * per, per, axis=0)
            w_down_in.append(lax.ppermute(away, 'tp', [(s, s ^ m) for s in range(TP)]))

        ids = jnp.arange(EXPERTS, dtype=jnp.int32)
        hit = jnp.any(topk_idx[:, :, None] == ids[None, None, :], axis=1)
        before = jnp.tril(jnp.ones((TOK, TOK), BF), -1)
        rank = dot(before, hit.astype(BF))
        rank = jnp.where(hit, rank, -1.0).astype(jnp.int32)
        slot_hit = rank[:, :, None] == jnp.arange(STRIP, dtype=jnp.int32)[None, None, :]
        token = jnp.arange(TOK, dtype=jnp.int32)[:, None, None] + 1
        table = jnp.sum(jnp.where(slot_hit, token, 0), axis=0, dtype=jnp.int32) - 1
        table = jnp.concatenate([table.reshape(EP, LOCAL * STRIP), jnp.zeros((8 - EP, LOCAL * STRIP), jnp.int32)], axis=0)
        all_rows, tables = gather_rows(jnp.concatenate([x, grad_y], axis=0), table)
        mine = lax.dynamic_index_in_dim(tables, ep, 1, keepdims=False).reshape(EP, TP, LOCAL, STRIP)
        base = (TOK * jnp.arange(EP, dtype=jnp.int32))[:, None, None, None]
        slots = jnp.where(mine >= 0, mine + base, -1).transpose(1, 2, 0, 3).reshape(TP, LOCAL * EP * STRIP, 1)

        parts, h, dab, xe, de = main_call(ep.reshape(1), all_rows, slots, w_router, ws_gate, ws_up, ws_down, permutations(), w_gate, w_up, w_down)
        summed = lax.psum_scatter(parts, 'tp', scatter_dimension=0).reshape(STEPS, BLK, D)

        h_in = []
        for m in range(1, TP):
            away = lax.dynamic_slice_in_dim(h, (tp ^ m) * per, per, axis=0)
            h_in.append(lax.ppermute(away, 'tp', [(s, s ^ m) for s in range(TP)]))
        o_send = out_call(tp.reshape(1), h, h_in, w_down, w_down_in)
        o_rows = lax.all_to_all(o_send, ('ep', 'tp'), 0, 0).reshape(EXPERTS * STRIP, D)

        d_w_gate, d_w_up, d_w_down = grad_call(xe, de, h, dab)

        x_all = all_rows[:, :TOK].reshape(NDEV * TOK, D)
        gy_all = all_rows[:, TOK:].reshape(NDEV * TOK, D)
        sa = dot(x_all, ws_gate).astype(BF).astype(F32)
        sb = dot(x_all, ws_up).astype(BF).astype(F32)
        sdh = dot_nt(gy_all, ws_down).astype(BF).astype(F32)
        s_h, s_da, s_db = act_both(sa, sb, sdh)
        ds_gate = dot_tn(x_all, s_da)
        ds_up = dot_tn(x_all, s_db)
        ds_down = dot_tn(s_h, gy_all)

        probs = jax.nn.softmax(dot(x, w_router), axis=-1)
        scaled = GATE_SCALE * probs
        gate_slot = jnp.where(slot_hit, scaled[:, :, None], 0.0).reshape(TOK, EXPERTS * STRIP)
        routed = jnp.dot(gate_slot, o_rows.astype(F32), precision=lax.Precision.HIGHEST)
        seen = dot_nt(grad_y, o_rows).reshape(TOK, EXPERTS, STRIP)
        d_scores = GATE_SCALE * jnp.sum(jnp.where(slot_hit, seen, 0.0), axis=2)
        d_logits = probs * (d_scores - jnp.sum(probs * d_scores, axis=-1, keepdims=True))
        d_logits_all = lax.all_gather(d_logits, ('ep', 'tp'), axis=0, tiled=True)
        d_router = lax.dot_general(x_all.astype(F32), d_logits_all, (((0,), (0,)), ((), ())), precision=lax.Precision.HIGHEST)
        dx_router = lax.dot_general(d_logits, w_router.astype(F32), (((1,), (1,)), ((), ())), precision=lax.Precision.HIGHEST)

        half = STEPS // 2
        shared = summed[:half, PAIR_ROWS:].reshape(TOK, D)
        dx_shared = summed[half:, PAIR_ROWS:].reshape(TOK, D)
        y_out = (shared + routed).astype(BF)
        own = summed[:, :PAIR_ROWS].astype(BF).reshape(STEPS, EP, 2 * CAP, D).transpose(1, 0, 2, 3)
        back = lax.all_to_all(own, 'ep', 0, 0).reshape(EXPERTS * CAP, D)
        mark = slot_hit[:, :, :CAP].reshape(TOK, EXPERTS * CAP).astype(BF)
        dx_out = (dx_router + dx_shared + dot(mark, back)).astype(BF)
        return y_out, dx_out, d_router, d_w_gate, d_w_up, d_w_down, ds_gate, ds_up, ds_down

    tok_spec = P(('ep', 'tp'), None)
    in_specs = (tok_spec, tok_spec, P(None, None), P('ep', None, 'tp'), P('ep', None, 'tp'), P('ep', 'tp', None), P(None, 'tp'), P(None, 'tp'), P('tp', None), tok_spec)
    out_specs = (tok_spec, tok_spec, P(None, None), P('ep', None, 'tp'), P('ep', None, 'tp'), P('ep', 'tp', None), P(None, 'tp'), P(None, 'tp'), P('tp', None))
    return jax.shard_map(device_step, mesh=mesh, in_specs=in_specs, out_specs=out_specs, check_vma=False)
```

```python
import jax
import jax.numpy as jnp
from jax import lax
from jax.experimental import pallas as pl
from jax.experimental.pallas import tpu as pltpu
from jax.sharding import PartitionSpec as P


GATE_SCALE = 16.0
BF = jnp.bfloat16
F32 = jnp.float32
MESH = pl.DeviceIdType.MESH

D = 1536
EXPERTS = 64
TOK = 64
TP = 4
EP = 4
NDEV = TP * EP
LOCAL = EXPERTS // EP
CAP = 7
STRIP = 8
ROWS = NDEV * STRIP
PAIR_ROWS = 2 * EP * CAP
STEPS = LOCAL // 2
SH_ROWS = 2 * TOK // STEPS
BLK = PAIR_ROWS + SH_ROWS
CHUNKS = 2
PER_CHUNK = STEPS // CHUNKS
EARLY = 2

BIT_Y, BIT_Z, BIT_C, BIT_X = 1, 2, 4, 8


def flip(value, bit):
    return value + bit * (1 - 2 * ((value // bit) % 2))


def flip_mask(value, mask):
    for bit in (1, 2, 4, 8):
        if mask & bit:
            value = flip(value, bit)
    return value


def dot(a, b):
    return jnp.dot(a, b, preferred_element_type=F32)


def dot_nt(a, b):
    return lax.dot_general(a, b, (((1,), (1,)), ((), ())), preferred_element_type=F32)


def dot_tn(a, b):
    return lax.dot_general(a, b, (((0,), (0,)), ((), ())), preferred_element_type=F32)


def act_both(a, b, dh):
    sig = 1.0 / (1.0 + jnp.exp(-a))
    silu = a * sig
    h = (silu * b).astype(BF)
    db = (dh * silu).astype(BF)
    da = (dh * b * (sig * (1.0 + a * (1.0 - sig)))).astype(BF)
    return h, da, db


def gather_kernel(rows_ref, tab_ref, w_ref, all_ref, tabs_ref, w_in_ref, keep_ref, send_sem, recv_sem, local_sem, w_send, w_recv, keep_sem):
    tp = lax.axis_index('tp')
    ep = lax.axis_index('ep')
    me = ep * TP + tp
    third = D // 3

    def peer(mask):
        return (flip_mask(tp, mask & 3), flip_mask(ep, mask >> 2))

    barrier = pltpu.get_barrier_semaphore()
    for mask in (BIT_X, BIT_Y, BIT_Z, BIT_C, BIT_Y | BIT_Z):
        pl.semaphore_signal(barrier, inc=1, device_id=peer(mask), device_id_type=MESH)
    pl.semaphore_wait(barrier, 5)

    sent = []
    for m in range(1, TP):
        first = flip_mask(tp, m) * (LOCAL // TP)
        c = pltpu.make_async_remote_copy(src_ref=w_ref.at[pl.ds(first, EARLY)], dst_ref=w_in_ref.at[m - 1],
                                         send_sem=w_send.at[m - 1], recv_sem=w_recv.at[m - 1], device_id=peer(m), device_id_type=MESH)
        c.start()
        sent.append(c)

    orders = [(BIT_X, BIT_Y, BIT_Z), (BIT_Y, BIT_Z, BIT_X), (BIT_Z, BIT_X, BIT_Y), (BIT_X, BIT_Y, BIT_Z)]

    def view(part, block, own):
        if part == 3:
            return tab_ref if own else tabs_ref.at[block]
        cols = pl.ds(part * third, third)
        return rows_ref.at[:, cols] if own else all_ref.at[block, :, cols]

    def copy(part, k, mask):
        block = flip_mask(me, k)
        return pltpu.make_async_remote_copy(
            src_ref=view(part, block, k == 0), dst_ref=view(part, block, False),
            send_sem=send_sem.at[part, k ^ mask], recv_sem=recv_sem.at[part, k ^ mask],
            device_id=peer(mask), device_id_type=MESH)

    def send(part, k, mask):
        c = copy(part, k, mask)
        c.start()
        sent.append(c)

    def arrived(part, k):
        block = flip_mask(me, k)
        pltpu.make_async_remote_copy(
            src_ref=view(part, block, False), dst_ref=view(part, block, False),
            send_sem=send_sem.at[part, k], recv_sem=recv_sem.at[part, k],
            device_id=peer(BIT_C), device_id_type=MESH).wait_recv()

    parts = (3, 0, 1, 2)
    for step in range(3):
        for part in parts:
            send(part, 0, orders[part][step])
    for part in parts:
        send(part, 0, BIT_C)
    own_rows = pltpu.make_async_copy(rows_ref, all_ref.at[me], local_sem.at[0])
    own_tab = pltpu.make_async_copy(tab_ref, tabs_ref.at[me], local_sem.at[1])
    own_rows.start()
    own_tab.start()
    for part in parts:
        m1, m2, m3 = orders[part]
        arrived(part, m1)
        send(part, m1, m2)
        send(part, m1, m3)
        send(part, m1, BIT_C)
    for part in parts:
        m1, m2, m3 = orders[part]
        arrived(part, m2)
        send(part, m2, m3)
        send(part, m2, BIT_C)
    for part in parts:
        m1, m2, m3 = orders[part]
        arrived(part, m1 ^ m2)
        send(part, m1 ^ m2, m3)
        send(part, m1 ^ m2, BIT_C)
    for extra in range(4):
        for part in parts:
            m1, m2, m3 = orders[part]
            k = (m3, m1 ^ m3, m2 ^ m3, m1 ^ m2 ^ m3)[extra]
            arrived(part, k)
            send(part, k, BIT_C)
    own_rows.wait()
    own_tab.wait()
    kept = []
    for k in sorted(range(16), key=lambda k: k & BIT_C):
        if k & BIT_C:
            for part in parts:
                arrived(part, k)
        block = flip_mask(me, k)
        c = pltpu.make_async_copy(all_ref.at[block], keep_ref.at[block], keep_sem.at[k])
        c.start()
        kept.append(c)
    for c in kept:
        c.wait()
    for c in sent[:TP - 1]:
        c.wait_recv()
    for c in sent:
        c.wait_send()


def gather_rows(rows, tab, w_down):
    vmem = pl.BlockSpec(memory_space=pltpu.VMEM)
    hbm = pl.BlockSpec(memory_space=pltpu.HBM)
    return pl.pallas_call(
        gather_kernel,
        name='gather_rows',
        out_shape=(jax.ShapeDtypeStruct((NDEV,) + rows.shape, rows.dtype), jax.ShapeDtypeStruct((NDEV,) + tab.shape, tab.dtype),
                   jax.ShapeDtypeStruct((TP - 1, EARLY) + w_down.shape[1:], w_down.dtype), jax.ShapeDtypeStruct((NDEV,) + rows.shape, rows.dtype)),
        in_specs=[vmem, vmem, hbm],
        out_specs=(vmem, vmem, hbm, hbm),
        scratch_shapes=[pltpu.SemaphoreType.DMA((4, 16)), pltpu.SemaphoreType.DMA((4, 16)), pltpu.SemaphoreType.DMA((2,)),
                        pltpu.SemaphoreType.DMA((TP - 1,)), pltpu.SemaphoreType.DMA((TP - 1,)), pltpu.SemaphoreType.DMA((NDEV,))],
        compiler_params=pltpu.CompilerParams(collective_id=0, has_side_effects=True, vmem_limit_bytes=40 << 20),
        cost_estimate=pl.CostEstimate(flops=40_000_000_000, bytes_accessed=7_000_000, transcendentals=0),
    )(rows, tab, w_down)


def chunk_members(chunk):
    return ((0, 1), (2, 3)) if chunk % 2 == 0 else ((0, 2), (1, 3))


def main_kernel(g_ref, all_ref, slot_ref, wr_ref, wsg_ref, wsu_ref, wsd_ref, perm_ref, wg_ref, wu_ref, wd_ref, *refs):
    chunk_refs, (h_ref, dab_ref, xe_hbm, de_hbm, xe, de, sh, sems) = refs[:2 * CHUNKS], refs[2 * CHUNKS:]
    step = pl.program_id(0)
    g = g_ref[0]
    tp = g_ref[1]
    third = D // 3
    xe_copy = pltpu.make_async_copy(xe, xe_hbm, sems.at[0])
    de_copy = pltpu.make_async_copy(de, de_hbm, sems.at[1])

    @pl.when(step == 0)
    def _():
        n_rows = LOCAL * EP * STRIP
        lane = lax.broadcasted_iota(jnp.int32, (n_rows, EP * TOK), 1)
        wr = wr_ref[...]
        row_expert = g * LOCAL + lax.broadcasted_iota(jnp.int32, (n_rows, 3 * EXPERTS), 0) // (EP * STRIP)
        wanted = lax.broadcasted_iota(jnp.int32, (n_rows, 3 * EXPERTS), 1) % EXPERTS == row_expert
        for j in range(TP):
            pick = jnp.where(slot_ref[j] == lane, 1.0, 0.0).astype(BF)
            x_j = jnp.concatenate([all_ref[s * TP + j, :TOK, :] for s in range(EP)], axis=0)
            logits = dot(x_j, wr)
            top = jnp.max(logits, axis=-1, keepdims=True)
            ex = jnp.exp(logits - top)
            probs = ex / jnp.sum(ex, axis=-1, keepdims=True)
            hi = probs.astype(BF)
            rest = probs - hi.astype(F32)
            mid = rest.astype(BF)
            low = (rest - mid.astype(F32)).astype(BF)
            sel = dot(pick, jnp.concatenate([hi, mid, low], axis=1))
            gate = GATE_SCALE * jnp.sum(jnp.where(wanted, sel, 0.0), axis=1, keepdims=True)
            for n in range(3):
                cols = slice(n * third, (n + 1) * third)
                got = dot(pick, x_j[:, cols]).astype(BF)
                xe[:, EP * STRIP * j:EP * STRIP * (j + 1), cols] = got.reshape(LOCAL, EP * STRIP, third)
                gy_j = jnp.concatenate([all_ref[s * TP + j, TOK:, cols] for s in range(EP)], axis=0)
                got = (dot(pick, gy_j) * gate).astype(BF)
                de[:, EP * STRIP * j:EP * STRIP * (j + 1), cols] = got.reshape(LOCAL, EP * STRIP, third)
        xe_copy.start()
        de_copy.start()
        x_s = jnp.concatenate([all_ref[g * TP + j, :TOK, :] for j in range(TP)], axis=0)
        gy_s = jnp.concatenate([all_ref[g * TP + j, TOK:, :] for j in range(TP)], axis=0)
        a = dot(x_s, wsg_ref[...]).astype(BF).astype(F32)
        b = dot(x_s, wsu_ref[...]).astype(BF).astype(F32)
        dh = dot_nt(gy_s, wsd_ref[...]).astype(BF).astype(F32)
        h, da, db = act_both(a, b, dh)
        for n in range(3):
            cols = slice(n * third, (n + 1) * third)
            sh[0, :, :, cols] = dot(h, wsd_ref[:, cols]).reshape(TP, TOK, third)
            dxs = dot_nt(da, wsg_ref[cols, :]) + dot_nt(db, wsu_ref[cols, :])
            sh[1, :, :, cols] = dxs.reshape(TP, TOK, third)

    lhs = []
    for i in range(2):
        e = 2 * step + i
        x_e = xe[e]
        ab = dot(x_e, jnp.concatenate([wg_ref[i], wu_ref[i]], axis=1)).astype(BF).astype(F32)
        dh = dot_nt(de[e], wd_ref[i]).astype(BF).astype(F32)
        width = ab.shape[1] // 2
        h, da, db = act_both(ab[:, :width], ab[:, width:], dh)
        h_ref[i] = h
        dab = jnp.concatenate([da, db], axis=1)
        dab_ref[i] = dab
        lhs.append(dot(perm_ref[i], dab).astype(BF))
    lhs = jnp.concatenate(lhs, axis=1)
    half = step // (STEPS // 2)
    first = pl.multiple_of((step % (STEPS // 2)) * SH_ROWS, SH_ROWS)
    found = []
    for n in range(3):
        cols = slice(n * third, (n + 1) * third)
        rhs = jnp.concatenate([wg_ref[0, cols, :], wu_ref[0, cols, :], wg_ref[1, cols, :], wu_ref[1, cols, :]], axis=1)
        found.append(dot_nt(lhs, rhs).reshape(TP, PAIR_ROWS, third))
    for chunk in range(CHUNKS):
        @pl.when(step // (STEPS // CHUNKS) == chunk)
        def _(chunk=chunk):
            for ref, members in zip(chunk_refs[2 * chunk:2 * chunk + 2], chunk_members(chunk)):
                for at, rel in enumerate(members):
                    for n in range(3):
                        ref[at, :PAIR_ROWS, n * third:(n + 1) * third] = found[n][rel]
                    away = rel ^ tp
                    ref[at, PAIR_ROWS:, :] = sh[half, away, pl.ds(first, SH_ROWS), :]

    @pl.when(step == STEPS - 1)
    def _():
        xe_copy.wait()
        de_copy.wait()


def main_call(g, all_rows, slots, w_router, ws_gate, ws_up, ws_down, perm, w_gate, w_up, w_down):
    width = w_gate.shape[2]

    def whole(a):
        return pl.BlockSpec(a.shape, lambda i, g_: (0,) * a.ndim, pipeline_mode=pl.Buffered(1))

    def pair(a):
        return pl.BlockSpec((2,) + a.shape[1:], lambda i, g_: (i, 0, 0))

    any_spec = pl.BlockSpec(memory_space=pl.ANY)
    chunk_specs = [pl.BlockSpec((2, BLK, D), lambda i, g_, c=n // 2: (0, jnp.clip(i - PER_CHUNK * c, 0, PER_CHUNK - 1), 0))
                   for n in range(2 * CHUNKS)]
    return pl.pallas_call(
        main_kernel,
        name='main_call',
        grid_spec=pltpu.PrefetchScalarGridSpec(
            num_scalar_prefetch=1,
            grid=(STEPS,),
            in_specs=[pl.BlockSpec(memory_space=pltpu.VMEM), whole(slots), whole(w_router), whole(ws_gate), whole(ws_up), whole(ws_down), whole(perm),
                      pair(w_gate), pair(w_up), pair(w_down)],
            out_specs=chunk_specs + [
                       pl.BlockSpec((2, ROWS, width), lambda i, g_: (i, 0, 0)),
                       pl.BlockSpec((2, ROWS, 2 * width), lambda i, g_: (i, 0, 0)), any_spec, any_spec],
            scratch_shapes=[pltpu.VMEM((LOCAL, ROWS, D), BF), pltpu.VMEM((LOCAL, ROWS, D), BF),
                            pltpu.VMEM((2, TP, TOK, D), F32), pltpu.SemaphoreType.DMA((2,))],
        ),
        out_shape=[jax.ShapeDtypeStruct((2, BLK * PER_CHUNK, D), F32)] * (2 * CHUNKS) + [
                   jax.ShapeDtypeStruct((LOCAL, ROWS, width), BF),
                   jax.ShapeDtypeStruct((LOCAL, ROWS, 2 * width), BF),
                   jax.ShapeDtypeStruct((LOCAL, ROWS, D), BF), jax.ShapeDtypeStruct((LOCAL, ROWS, D), BF)],
        compiler_params=pltpu.CompilerParams(vmem_limit_bytes=48 << 20),
        cost_estimate=pl.CostEstimate(flops=20_000_000_000, bytes_accessed=60_000_000, transcendentals=4_000_000),
    )(g, all_rows, slots, w_router, ws_gate, ws_up, ws_down, perm, w_gate, w_up, w_down)


def grad_kernel(xe_ref, de_ref, h_ref, dab_ref, dg_ref, du_ref, dd_ref):
    both = dot_tn(xe_ref[0], dab_ref[0])
    width = both.shape[1] // 2
    dg_ref[0] = both[:, :width]
    du_ref[0] = both[:, width:]
    dd_ref[0] = dot_tn(h_ref[0], de_ref[0])


def grad_call(xe, de, h, dab):
    width = h.shape[2]

    def one(shape):
        return pl.BlockSpec((1,) + shape, lambda i: (i, 0, 0))

    return pl.pallas_call(
        grad_kernel,
        name='grad_call',
        grid=(LOCAL,),
        in_specs=[one((ROWS, D)), one((ROWS, D)), one((ROWS, width)), one((ROWS, 2 * width))],
        out_specs=[one((D, width)), one((D, width)), one((width, D))],
        out_shape=[jax.ShapeDtypeStruct((LOCAL, D, width), F32), jax.ShapeDtypeStruct((LOCAL, D, width), F32),
                   jax.ShapeDtypeStruct((LOCAL, width, D), F32)],
        compiler_params=pltpu.CompilerParams(vmem_limit_bytes=40 << 20),
        cost_estimate=pl.CostEstimate(flops=10_000_000_000, bytes_accessed=55_000_000, transcendentals=0),
    )(xe, de, h, dab)


def out_kernel(tp_ref, h0, h1, h2, h3, w_own, e1, e2, e3, l1, l2, l3, o_ref):
    def emit(e, w1, w2, w3):
        total = dot(jnp.concatenate([h0[0], h1[0], h2[0], h3[0]], axis=1), jnp.concatenate([w_own[0], w1, w2, w3], axis=0))
        for j in range(TP):
            for s in range(EP):
                first = STRIP * (j * EP + s)
                o_ref[s * TP + j, STRIP * e:STRIP * (e + 1), :] = total[first:first + STRIP].astype(BF)

    for e in range(LOCAL // TP):
        @pl.when(pl.program_id(0) == e)
        def _(e=e):
            if e < EARLY:
                emit(e, e1[0, 0], e2[0, 0], e3[0, 0])
            else:
                emit(e, l1[0], l2[0], l3[0])


def out_call(tp, h_own, h_in, w_down, w_early, w_late):
    width = h_own.shape[2]
    per = LOCAL // TP
    return pl.pallas_call(
        out_kernel,
        name='out_call',
        grid_spec=pltpu.PrefetchScalarGridSpec(
            num_scalar_prefetch=1,
            grid=(per,),
            in_specs=[pl.BlockSpec((1, ROWS, width), lambda i, t: (t[0] * per + i, 0, 0))] + [pl.BlockSpec((1, ROWS, width), lambda i, t: (i, 0, 0))] * 3
            + [pl.BlockSpec((1, width, D), lambda i, t: (t[0] * per + i, 0, 0))]
            + [pl.BlockSpec((1, 1, width, D), lambda i, t, m=m: (m, jnp.minimum(i, EARLY - 1), 0, 0)) for m in range(TP - 1)]
            + [pl.BlockSpec((1, width, D), lambda i, t: (jnp.maximum(i - EARLY, 0), 0, 0))] * 3,
            out_specs=pl.BlockSpec((NDEV, per * STRIP, D), lambda i, t: (0, 0, 0)),
        ),
        out_shape=jax.ShapeDtypeStruct((NDEV, per * STRIP, D), BF),
        compiler_params=pltpu.CompilerParams(vmem_limit_bytes=40 << 20),
        cost_estimate=pl.CostEstimate(flops=5_000_000_000, bytes_accessed=10_000_000, transcendentals=0),
    )(tp, h_own, *h_in, w_down, w_early, w_early, w_early, *w_late)


def split3(v):
    hi = v.astype(BF)
    rest = v - hi.astype(F32)
    mid = rest.astype(BF)
    return hi, mid, (rest - mid.astype(F32)).astype(BF)


def finish_kernel(keep0, keep1, first0, first1, o_ref, x_ref, gy_ref, wr_ref, mark_ref, mark16_ref, all_hbm,
                  y_ref, dx_ref, drt_ref,
                  k1, f1, k0, f0, snd, rcv, ret, ret_in, o_in, dl, xa, s_rows, d_rows,
                  load_sem, x_sem, s2_send, s2_recv, ret_send, ret_recv, o_send, o_recv, dl_send, dl_recv, local_sem):
    tp = lax.axis_index('tp')
    ep = lax.axis_index('ep')
    me = ep * TP + tp

    def peer(mask):
        return (flip_mask(tp, mask & 3), flip_mask(ep, mask >> 2))

    pieces = [(c, i) for i in range(PER_CHUNK) for c in range(CHUNKS)]
    loads = []
    for n, (c, i) in enumerate(pieces):
        rows = pl.ds(BLK * i, BLK)
        keep, first = (keep0, keep1)[c], (first0, first1)[c]
        loads.append([pltpu.make_async_copy(src, dst.at[n], load_sem.at[m, n]) for m, (src, dst) in enumerate((
            (keep.at[1, rows], k1), (first.at[1, rows], f1), (keep.at[0, rows], k0), (first.at[0, rows], f0)))])
    for group in (slice(0, 2), slice(2, 4)):
        for load in loads:
            for copy in load[group]:
                copy.start()
    x_load = pltpu.make_async_copy(all_hbm.at[:, pl.ds(0, TOK), :], xa, x_sem)
    x_load.start()

    barrier = pltpu.get_barrier_semaphore()
    for mask in range(1, NDEV):
        pl.semaphore_signal(barrier, inc=1, device_id=peer(mask), device_id_type=MESH)
    pl.semaphore_wait(barrier, NDEV - 1)

    sent = []

    def send(src, dst, sems, at, mask):
        copy = pltpu.make_async_remote_copy(src_ref=src, dst_ref=dst, send_sem=sems[0].at[at], recv_sem=sems[1].at[at],
                                            device_id=peer(mask), device_id_type=MESH)
        copy.start()
        sent.append(copy)

    def arrived(dst, sems, at):
        pltpu.make_async_remote_copy(src_ref=dst, dst_ref=dst, send_sem=sems[0].at[at], recv_sem=sems[1].at[at],
                                     device_id=peer(BIT_C), device_id_type=MESH).wait_recv()

    for mask in range(1, NDEV):
        send(o_ref.at[flip_mask(me, mask)], o_in.at[me], (o_send, o_recv), mask, mask)
    o_own = pltpu.make_async_copy(o_ref.at[me], o_in.at[me], local_sem)
    o_own.start()

    def second_stage(n):
        loads[n][0].wait()
        loads[n][1].wait()
        snd[n] = k1[n] + f1[n]
        send(snd.at[n], rcv.at[n], (s2_send, s2_recv), n, (BIT_Y, BIT_Z)[pieces[n][0]])

    for n in range(4):
        second_stage(n)

    x = x_ref[...]
    wr = wr_ref[...]
    logits = dot(x, wr)
    ex = jnp.exp(logits - jnp.max(logits, axis=-1, keepdims=True))
    probs = ex / jnp.sum(ex, axis=-1, keepdims=True)
    slots = EXPERTS * STRIP
    spread = (lax.broadcasted_iota(jnp.int32, (EXPERTS, slots), 1) // STRIP == lax.broadcasted_iota(jnp.int32, (EXPERTS, slots), 0))
    spread = jnp.where(spread, 1.0, 0.0).astype(BF)
    mark = mark_ref[...]
    hi, mid, low = split3(GATE_SCALE * probs)
    gate = (dot(hi, spread) + dot(mid, spread) + dot(low, spread)) * mark
    for mask in range(1, NDEV):
        arrived(o_in.at[flip_mask(me, mask)], (o_send, o_recv), mask)
    o_own.wait()
    o_rows = o_in[...].reshape(slots, D)
    hi, mid, low = split3(gate)
    routed = dot(hi, o_rows) + dot(mid, o_rows) + dot(low, o_rows)
    seen = dot_nt(gy_ref[...], o_rows) * mark
    hi, mid, low = split3(seen)
    d_scores = GATE_SCALE * (dot_nt(hi, spread) + dot_nt(mid, spread) + dot_nt(low, spread))
    d_logits = probs * (d_scores - jnp.sum(probs * d_scores, axis=-1, keepdims=True))
    dl[me] = jnp.concatenate([d_logits[:TOK // 2], d_logits[TOK // 2:]], axis=1)
    for mask in range(1, NDEV):
        send(dl.at[me], dl.at[me], (dl_send, dl_recv), mask, mask)
    for n in range(4, len(pieces)):
        second_stage(n)
    hi, mid, low = split3(d_logits)
    dx_router = dot_nt(hi, wr) + dot_nt(mid, wr) + dot_nt(low, wr)

    def finish_piece(n):
        c, i = pieces[n]
        arrived(rcv.at[n], (s2_send, s2_recv), n)
        loads[n][2].wait()
        loads[n][3].wait()
        own = k0[n] + f0[n] + rcv[n]
        for s in range(EP):
            rows = own[2 * CAP * s:2 * CAP * (s + 1)]
            ret[s, n] = jnp.concatenate([rows, jnp.zeros((16 - 2 * CAP, D), F32)], axis=0).astype(BF)
        for at, mask in enumerate((BIT_X, BIT_C, BIT_X | BIT_C)):
            send(ret.at[flip_mask(ep, mask >> 2), n], ret_in.at[ep, n], (ret_send, ret_recv), (n, at), mask)
        ret_in[ep, n] = ret[ep, n]
        (s_rows, d_rows)[c][SH_ROWS * i:SH_ROWS * (i + 1), :] = own[PAIR_ROWS:]

    for n in range(4):
        finish_piece(n)
    for mask in range(1, NDEV):
        arrived(dl.at[flip_mask(me, mask)], (dl_send, dl_recv), mask)
    x_load.wait()
    total = jnp.zeros((EXPERTS, D), F32)
    for half in range(2):
        x_half = xa[:, TOK // 2 * half:TOK // 2 * (half + 1), :].reshape(NDEV * TOK // 2, D)
        for part in split3(dl[...].reshape(NDEV * TOK // 2, 2 * EXPERTS)):
            total = total + dot_tn(part, x_half)[EXPERTS * half:EXPERTS * (half + 1)]
    drt_ref[...] = total
    for n in range(4, len(pieces)):
        finish_piece(n)
    y_ref[...] = (s_rows[...] + routed).astype(BF)
    for n in range(len(pieces)):
        for at, mask in enumerate((BIT_X, BIT_C, BIT_X | BIT_C)):
            arrived(ret_in.at[flip_mask(ep, mask >> 2), n], (ret_send, ret_recv), (n, at))
    back = ret_in[...].reshape(EP * STEPS * 16, D)
    dx_ref[...] = (dx_router + d_rows[...] + dot(mark16_ref[...], back)).astype(BF)
    for copy in sent:
        copy.wait_send()


def finish_call(keeps, firsts, o_send, x, grad_y, w_router, mark, mark16, all_rows):
    vmem = pl.BlockSpec(memory_space=pltpu.VMEM)
    anys = pl.BlockSpec(memory_space=pl.ANY)
    pieces = PER_CHUNK * CHUNKS
    piece = pltpu.VMEM((pieces, BLK, D), F32)
    ret = pltpu.VMEM((EP, pieces, 16, D), BF)
    dma = pltpu.SemaphoreType.DMA
    return pl.pallas_call(
        finish_kernel,
        name='finish_call',
        out_shape=(jax.ShapeDtypeStruct((TOK, D), BF), jax.ShapeDtypeStruct((TOK, D), BF), jax.ShapeDtypeStruct((EXPERTS, D), F32)),
        in_specs=[anys] * 4 + [vmem] * 6 + [anys],
        out_specs=(vmem, vmem, vmem),
        scratch_shapes=[piece] * 6 + [ret, ret, pltpu.VMEM((NDEV, LOCAL // TP * STRIP, D), BF), pltpu.VMEM((NDEV, TOK // 2, 2 * EXPERTS), F32),
                                      pltpu.VMEM((NDEV, TOK, D), BF), pltpu.VMEM((TOK, D), F32), pltpu.VMEM((TOK, D), F32),
                                      dma((4, pieces)), dma, dma((pieces,)), dma((pieces,)), dma((pieces, 3)), dma((pieces, 3)),
                                      dma((NDEV,)), dma((NDEV,)), dma((NDEV,)), dma((NDEV,)), dma],
        compiler_params=pltpu.CompilerParams(collective_id=1, has_side_effects=True, vmem_limit_bytes=48 << 20),
        cost_estimate=pl.CostEstimate(flops=50_000_000_000, bytes_accessed=20_000_000, transcendentals=0),
    )(*keeps, *firsts, o_send, x, grad_y, w_router, mark, mark16, all_rows)


def permutations(tp):
    row = jnp.arange(TP * PAIR_ROWS)
    col, rest = (row // PAIR_ROWS) ^ tp, row % PAIR_ROWS
    src, rest = rest // (2 * CAP), rest % (2 * CAP)
    which, slot = rest // CAP, rest % CAP
    wanted = col * (EP * STRIP) + src * STRIP + slot
    hit = wanted[:, None] == jnp.arange(ROWS)[None, :]
    return jnp.stack([hit & (which == i)[:, None] for i in range(2)]).astype(BF)


def solution(mesh):
    def device_body(x, grad_y, w_router, w_gate, w_up, w_down, ws_gate, ws_up, ws_down, topk_idx):
        tp = lax.axis_index('tp')
        ep = lax.axis_index('ep')
        per = LOCAL // TP
        ids = jnp.arange(EXPERTS, dtype=jnp.int32)
        hit = jnp.any(topk_idx[:, :, None] == ids[None, None, :], axis=1)
        before = jnp.tril(jnp.ones((TOK, TOK), BF), -1)
        rank = dot(before, hit.astype(BF))
        rank = jnp.where(hit, rank, -1.0).astype(jnp.int32)
        slot_hit = rank[:, :, None] == jnp.arange(STRIP, dtype=jnp.int32)[None, None, :]
        token = jnp.arange(TOK, dtype=jnp.int32)[:, None, None] + 1
        table = jnp.sum(jnp.where(slot_hit, token, 0), axis=0, dtype=jnp.int32) - 1
        table = jnp.concatenate([table.reshape(EP, LOCAL * STRIP), jnp.zeros((8 - EP, LOCAL * STRIP), jnp.int32)], axis=0)
        rows_near, tables, w_early, all_rows = gather_rows(jnp.concatenate([x, grad_y], axis=0), table, w_down)
        mine = lax.dynamic_index_in_dim(tables, ep, 1, keepdims=False).reshape(EP, TP, LOCAL, STRIP)
        w_late = []
        for m in range(1, TP):
            away = lax.dynamic_slice_in_dim(w_down, (tp ^ m) * per + EARLY, per - EARLY, axis=0)
            w_late.append(lax.ppermute(away, 'tp', [(s, s ^ m) for s in range(TP)]))
        base = (TOK * jnp.arange(EP, dtype=jnp.int32))[:, None, None, None]
        slots = jnp.where(mine >= 0, mine + base, -1).transpose(1, 2, 0, 3).reshape(TP, LOCAL * EP * STRIP, 1)

        *parts, h, dab, xe, de = main_call(jnp.stack([ep, tp]), rows_near, slots, w_router, ws_gate, ws_up, ws_down, permutations(tp), w_gate, w_up, w_down)
        h_in = []
        for m in range(1, TP):
            away = lax.dynamic_slice_in_dim(h, (tp ^ m) * per, per, axis=0)
            h_in.append(lax.ppermute(away, 'tp', [(s, s ^ m) for s in range(TP)]))
        firsts = [lax.ppermute(parts[2 * c + 1], 'tp', [(s, s ^ (2 - c)) for s in range(TP)]) for c in range(CHUNKS)]
        o_send = out_call(tp.reshape(1), h, h_in, w_down, w_early, w_late)

        d_w_gate, d_w_up, d_w_down = grad_call(xe, de, h, dab)

        x_all = all_rows[:, :TOK].reshape(NDEV * TOK, D)
        gy_all = all_rows[:, TOK:].reshape(NDEV * TOK, D)
        sa = dot(x_all, ws_gate).astype(BF).astype(F32)
        sb = dot(x_all, ws_up).astype(BF).astype(F32)
        sdh = dot_nt(gy_all, ws_down).astype(BF).astype(F32)
        s_h, s_da, s_db = act_both(sa, sb, sdh)
        ds_gate = dot_tn(x_all, s_da)
        ds_up = dot_tn(x_all, s_db)
        ds_down = dot_tn(s_h, gy_all)

        mark = slot_hit.reshape(TOK, EXPERTS * STRIP).astype(F32)
        mark16 = slot_hit[:, :, :CAP].reshape(TOK, EP, CHUNKS, PER_CHUNK, 2 * CAP).transpose(0, 1, 3, 2, 4)
        mark16 = jnp.pad(mark16, ((0, 0),) * 4 + ((0, 16 - 2 * CAP),)).reshape(TOK, EP * STEPS * 16).astype(BF)
        y_out, dx_out, d_router = finish_call(parts[0::2], firsts, o_send, x, grad_y, w_router, mark, mark16, all_rows)
        d_router = d_router.T
        return y_out, dx_out, d_router, d_w_gate, d_w_up, d_w_down, ds_gate, ds_up, ds_down

    tok_spec = P(('ep', 'tp'), None)
    in_specs = (tok_spec, tok_spec, P(None, None), P('ep', None, 'tp'), P('ep', None, 'tp'), P('ep', 'tp', None), P(None, 'tp'), P(None, 'tp'), P('tp', None), tok_spec)
    out_specs = (tok_spec, tok_spec, P(None, None), P('ep', None, 'tp'), P('ep', None, 'tp'), P('ep', 'tp', None), P(None, 'tp'), P(None, 'tp'), P('tp', None))
    return jax.shard_map(device_body, mesh=mesh, in_specs=in_specs, out_specs=out_specs, check_vma=False)
```

```python
import jax
import jax.numpy as jnp
import numpy as np
from jax import lax
from jax.experimental import pallas as pl
from jax.experimental.pallas import tpu as pltpu
from jax.sharding import PartitionSpec as P


GATE_SCALE = 16.0
BF = jnp.bfloat16
F32 = jnp.float32
MESH = pl.DeviceIdType.MESH

D = 1536
EXPERTS = 64
TOP = 6
TOK = 64
TP = 4
EP = 4
NDEV = TP * EP
LOCAL = EXPERTS // EP
CAP = 7
STRIP = 8
ROWS = NDEV * STRIP
PAIR_ROWS = 2 * EP * CAP
STEPS = LOCAL // 2
SH_ROWS = 2 * TOK // STEPS
BLK = PAIR_ROWS + SH_ROWS
CHUNKS = 2
PER_CHUNK = STEPS // CHUNKS

BIT_Y, BIT_Z, BIT_C, BIT_X = 1, 2, 4, 8


def flip(value, bit):
    return value + bit * (1 - 2 * ((value // bit) % 2))


def flip_mask(value, mask):
    for bit in (1, 2, 4, 8):
        if mask & bit:
            value = flip(value, bit)
    return value


def dot(a, b):
    return jnp.dot(a, b, preferred_element_type=F32)


def dot_nt(a, b):
    return lax.dot_general(a, b, (((1,), (1,)), ((), ())), preferred_element_type=F32)


def dot_tn(a, b):
    return lax.dot_general(a, b, (((0,), (0,)), ((), ())), preferred_element_type=F32)


def act_both(a, b, dh):
    sig = 1.0 / (1.0 + jnp.exp(-a))
    silu = a * sig
    h = (silu * b).astype(BF)
    db = (dh * silu).astype(BF)
    da = (dh * b * (sig * (1.0 + a * (1.0 - sig)))).astype(BF)
    return h, da, db


def gather_rows(x_ref, gy_ref, tab_ref, w_ref, all_ref, tabs_ref, w_in_ref, keep_ref, send_sem, recv_sem, local_sem, w_send, w_recv, keep_sem):
    tp = lax.axis_index('tp')
    ep = lax.axis_index('ep')
    me = ep * TP + tp
    third = D // 3

    def peer(mask):
        return (flip_mask(tp, mask & 3), flip_mask(ep, mask >> 2))

    own = [pltpu.make_async_copy(x_ref, all_ref.at[me, pl.ds(0, TOK)], local_sem.at[0]),
           pltpu.make_async_copy(gy_ref, all_ref.at[me, pl.ds(TOK, TOK)], local_sem.at[1]),
           pltpu.make_async_copy(tab_ref, tabs_ref.at[me], local_sem.at[2])]
    for c in own:
        c.start()
    barrier = pltpu.get_barrier_semaphore()
    for mask in (BIT_X, BIT_Y, BIT_Z, BIT_C, BIT_Y | BIT_Z):
        pl.semaphore_signal(barrier, inc=1, device_id=peer(mask), device_id_type=MESH)
    pl.semaphore_wait(barrier, 5)
    for c in own:
        c.wait()

    orders = [(BIT_Y, BIT_Z, BIT_X), (BIT_Z, BIT_Y, BIT_X), (BIT_Y, BIT_Z, BIT_X), (BIT_Z, BIT_Y, BIT_X)]

    def view(part, block):
        if part == 3:
            return tabs_ref.at[block]
        return all_ref.at[block, :, pl.ds(part * third, third)]

    sent = []

    def send(part, k, mask):
        block = flip_mask(me, k)
        c = pltpu.make_async_remote_copy(
            src_ref=view(part, block), dst_ref=view(part, block),
            send_sem=send_sem.at[part, k ^ mask], recv_sem=recv_sem.at[part, k ^ mask],
            device_id=peer(mask), device_id_type=MESH)
        c.start()
        sent.append(c)

    def arrived(part, k):
        block = flip_mask(me, k)
        pltpu.make_async_remote_copy(
            src_ref=view(part, block), dst_ref=view(part, block),
            send_sem=send_sem.at[part, k], recv_sem=recv_sem.at[part, k],
            device_id=peer(BIT_C), device_id_type=MESH).wait_recv()

    parts = (3, 0, 1, 2)
    for step in range(3):
        for part in parts:
            send(part, 0, orders[part][step])
    for part in parts:
        send(part, 0, BIT_C)
    for part in parts:
        m1, m2, m3 = orders[part]
        arrived(part, m1)
        send(part, m1, m2)
        send(part, m1, m3)
        send(part, m1, BIT_C)
    per = LOCAL // TP
    for m in range(1, TP):
        c = pltpu.make_async_remote_copy(src_ref=w_ref.at[pl.ds(flip_mask(tp, m) * per, per)], dst_ref=w_in_ref.at[m - 1],
                                         send_sem=w_send.at[m - 1], recv_sem=w_recv.at[m - 1], device_id=peer(m), device_id_type=MESH)
        c.start()
    for part in parts:
        m1, m2, m3 = orders[part]
        arrived(part, m2)
        send(part, m2, m3)
        send(part, m2, BIT_C)
    for part in parts:
        m1, m2, m3 = orders[part]
        arrived(part, m1 ^ m2)
        send(part, m1 ^ m2, m3)
        send(part, m1 ^ m2, BIT_C)
    for extra in range(4):
        for part in parts:
            m1, m2, m3 = orders[part]
            k = (m3, m1 ^ m3, m2 ^ m3, m1 ^ m2 ^ m3)[extra]
            arrived(part, k)
            send(part, k, BIT_C)
    kept = []
    for k in sorted(range(16), key=lambda k: k & BIT_C):
        if k & BIT_C:
            for part in parts:
                arrived(part, k)
        block = flip_mask(me, k)
        c = pltpu.make_async_copy(all_ref.at[block], keep_ref.at[block], keep_sem.at[k])
        c.start()
        kept.append(c)
    for c in kept:
        c.wait()
    for c in sent:
        c.wait_send()


def split3(v):
    hi = v.astype(BF)
    rest = v - hi.astype(F32)
    mid = rest.astype(BF)
    return hi, mid, (rest - mid.astype(F32)).astype(BF)


def chunk_members(chunk):
    return ((0, 1), (2, 3)) if chunk % 2 == 0 else ((0, 2), (1, 3))


def main_kernel(x_ref, gy_ref, tab_ref, w_all_ref, wr_ref, wsg_ref, wsu_ref, wsd_ref, perm_ref, wg_ref, wu_ref, wd_ref, *refs):
    chunk_refs, refs = refs[:2 * CHUNKS], refs[2 * CHUNKS:]
    (h_ref, dab_ref, xe_hbm, de_hbm, w_in_ref, keep_ref, h_in_ref, all_ref, tabs_ref, xe, de, sh, hs, sems,
     send_sem, recv_sem, local_sem, w_send, w_recv, keep_sem, h_send, h_recv) = refs
    step = pl.program_id(0)
    g = lax.axis_index('ep')
    tp = lax.axis_index('tp')
    third = D // 3
    per = LOCAL // TP
    xe_copy = pltpu.make_async_copy(xe, xe_hbm, sems.at[0])
    de_copy = pltpu.make_async_copy(de, de_hbm, sems.at[1])

    @pl.when(step == 0)
    def _():
        gather_rows(x_ref, gy_ref, tab_ref, w_all_ref, all_ref, tabs_ref, w_in_ref, keep_ref, send_sem, recv_sem, local_sem, w_send, w_recv, keep_sem)
        n_rows = LOCAL * EP * STRIP
        expert = g * LOCAL + lax.broadcasted_iota(jnp.int32, (LOCAL, TOK), 0)
        early = lax.broadcasted_iota(jnp.int32, (EP * TOK, EP * TOK), 0)
        late = lax.broadcasted_iota(jnp.int32, (EP * TOK, EP * TOK), 1)
        before = jnp.where((early < late) & (early // TOK == late // TOK), 1.0, 0.0).astype(BF)
        cube = (LOCAL, EP * STRIP, EP * TOK)
        place = lax.broadcasted_iota(jnp.int32, cube, 1)
        wanted_rank = (place % STRIP).astype(F32)
        same_source = place // STRIP == lax.broadcasted_iota(jnp.int32, cube, 2) // TOK
        wr = wr_ref[...]
        row_expert = g * LOCAL + lax.broadcasted_iota(jnp.int32, (n_rows, 3 * EXPERTS), 0) // (EP * STRIP)
        wanted = lax.broadcasted_iota(jnp.int32, (n_rows, 3 * EXPERTS), 1) % EXPERTS == row_expert
        for j in range(TP):
            hit = []
            for s in range(EP):
                ids = tabs_ref[s * TP + j]
                found = ids[0:1, :] == expert
                for k in range(1, TOP):
                    found = found | (ids[k:k + 1, :] == expert)
                hit.append(jnp.where(found, 1.0, 0.0))
            hit = jnp.concatenate(hit, axis=1)
            rank = jnp.where(hit > 0.0, dot(hit.astype(BF), before), -1.0)
            rank = jnp.broadcast_to(rank[:, None, :], cube)
            pick = jnp.where((rank == wanted_rank) & same_source, 1.0, 0.0).reshape(n_rows, EP * TOK).astype(BF)
            x_j = jnp.concatenate([all_ref[s * TP + j, :TOK, :] for s in range(EP)], axis=0)
            logits = dot_nt(x_j, wr)
            top = jnp.max(logits, axis=-1, keepdims=True)
            ex = jnp.exp(logits - top)
            probs = ex / jnp.sum(ex, axis=-1, keepdims=True)
            sel = dot(pick, jnp.concatenate(split3(probs), axis=1))
            gate = GATE_SCALE * jnp.sum(jnp.where(wanted, sel, 0.0), axis=1, keepdims=True)
            for n in range(3):
                cols = slice(n * third, (n + 1) * third)
                got = dot(pick, x_j[:, cols]).astype(BF)
                xe[:, EP * STRIP * j:EP * STRIP * (j + 1), cols] = got.reshape(LOCAL, EP * STRIP, third)
                gy_j = jnp.concatenate([all_ref[s * TP + j, TOK:, cols] for s in range(EP)], axis=0)
                got = (dot(pick, gy_j) * gate).astype(BF)
                de[:, EP * STRIP * j:EP * STRIP * (j + 1), cols] = got.reshape(LOCAL, EP * STRIP, third)
        xe_copy.start()
        de_copy.start()
        x_s = jnp.concatenate([all_ref[g * TP + j, :TOK, :] for j in range(TP)], axis=0)
        gy_s = jnp.concatenate([all_ref[g * TP + j, TOK:, :] for j in range(TP)], axis=0)
        a = dot(x_s, wsg_ref[...]).astype(BF).astype(F32)
        b = dot(x_s, wsu_ref[...]).astype(BF).astype(F32)
        dh = dot_nt(gy_s, wsd_ref[...]).astype(BF).astype(F32)
        h, da, db = act_both(a, b, dh)
        for n in range(3):
            cols = slice(n * third, (n + 1) * third)
            sh[0, :, :, cols] = dot(h, wsd_ref[:, cols]).reshape(TP, TOK, third)
            dxs = dot_nt(da, wsg_ref[cols, :]) + dot_nt(db, wsu_ref[cols, :])
            sh[1, :, :, cols] = dxs.reshape(TP, TOK, third)

    lhs = []
    for i in range(2):
        e = 2 * step + i
        x_e = xe[e]
        ab = dot(x_e, jnp.concatenate([wg_ref[i], wu_ref[i]], axis=1)).astype(BF).astype(F32)
        dh = dot_nt(de[e], wd_ref[i]).astype(BF).astype(F32)
        width = ab.shape[1] // 2
        h, da, db = act_both(ab[:, :width], ab[:, width:], dh)
        h_ref[i] = h
        hs[e] = h
        dab = jnp.concatenate([da, db], axis=1)
        dab_ref[i] = dab
        dab = jnp.concatenate([dab_ref[i, pl.ds(pl.multiple_of(flip_mask(tp, rel) * EP * STRIP, EP * STRIP), EP * STRIP), :] for rel in range(TP)], axis=0)
        lhs.append(dot(perm_ref[i], dab).astype(BF))
    lhs = jnp.concatenate(lhs, axis=1)
    half = step // (STEPS // 2)
    first = pl.multiple_of((step % (STEPS // 2)) * SH_ROWS, SH_ROWS)
    found = []
    for n in range(3):
        cols = slice(n * third, (n + 1) * third)
        rhs = jnp.concatenate([wg_ref[0, cols, :], wu_ref[0, cols, :], wg_ref[1, cols, :], wu_ref[1, cols, :]], axis=1)
        found.append(dot_nt(lhs, rhs).reshape(TP, PAIR_ROWS, third))
    for chunk in range(CHUNKS):
        @pl.when(step // (STEPS // CHUNKS) == chunk)
        def _(chunk=chunk):
            for ref, members in zip(chunk_refs[2 * chunk:2 * chunk + 2], chunk_members(chunk)):
                for at, rel in enumerate(members):
                    for n in range(3):
                        ref[at, :PAIR_ROWS, n * third:(n + 1) * third] = found[n][rel]
                    away = flip_mask(tp, rel)
                    ref[at, PAIR_ROWS:, :] = sh[half, away, pl.ds(first, SH_ROWS), :]

    @pl.when(step == STEPS - 1)
    def _():
        h_copies = []
        for m in range(1, TP):
            to = flip_mask(tp, m)
            c = pltpu.make_async_remote_copy(src_ref=hs.at[pl.ds(to * per, per)], dst_ref=h_in_ref.at[m - 1],
                                             send_sem=h_send.at[m - 1], recv_sem=h_recv.at[m - 1], device_id=(to, g), device_id_type=MESH)
            c.start()
            h_copies.append(c)
        xe_copy.wait()
        de_copy.wait()
        for m in range(1, TP):
            to = flip_mask(tp, m)
            pltpu.make_async_remote_copy(src_ref=w_all_ref.at[pl.ds(to * per, per)], dst_ref=w_in_ref.at[m - 1],
                                         send_sem=w_send.at[m - 1], recv_sem=w_recv.at[m - 1], device_id=(to, g), device_id_type=MESH).wait()
        for c in h_copies:
            c.wait()


def main_call(x, grad_y, table, w_router, ws_gate, ws_up, ws_down, perm, w_gate, w_up, w_down):
    width = w_gate.shape[2]
    per = LOCAL // TP

    def whole(a):
        return pl.BlockSpec(a.shape, lambda i: (0,) * a.ndim, pipeline_mode=pl.Buffered(1))

    def pair(a):
        return pl.BlockSpec((2,) + a.shape[1:], lambda i: (i, 0, 0))

    hbm = pl.BlockSpec(memory_space=pltpu.HBM)
    vmem = pl.BlockSpec(memory_space=pltpu.VMEM)
    dma = pltpu.SemaphoreType.DMA
    chunk_specs = [pl.BlockSpec((2, BLK, D), lambda i, c=n // 2: (0, jnp.clip(i - PER_CHUNK * c, 0, PER_CHUNK - 1), 0))
                   for n in range(2 * CHUNKS)]
    return pl.pallas_call(
        main_kernel,
        name='main_call',
        grid=(STEPS,),
        in_specs=[vmem, vmem, vmem, hbm, whole(w_router), whole(ws_gate), whole(ws_up), whole(ws_down), whole(perm),
                  pair(w_gate), pair(w_up), pair(w_down)],
        out_specs=chunk_specs + [
            pl.BlockSpec((2, ROWS, width), lambda i: (i, 0, 0)),
            pl.BlockSpec((2, ROWS, 2 * width), lambda i: (i, 0, 0)), hbm, hbm, hbm, hbm, hbm],
        scratch_shapes=[pltpu.VMEM((NDEV, 2 * TOK, D), BF), pltpu.VMEM((NDEV,) + table.shape, jnp.int32),
                        pltpu.VMEM((LOCAL, ROWS, D), BF), pltpu.VMEM((LOCAL, ROWS, D), BF),
                        pltpu.VMEM((2, TP, TOK, D), F32), pltpu.VMEM((LOCAL, ROWS, width), BF), dma((2,)),
                        dma((4, 16)), dma((4, 16)), dma((3,)), dma((TP - 1,)), dma((TP - 1,)), dma((NDEV,)), dma((TP - 1,)), dma((TP - 1,))],
        out_shape=[jax.ShapeDtypeStruct((2, BLK * PER_CHUNK, D), F32)] * (2 * CHUNKS) + [
            jax.ShapeDtypeStruct((LOCAL, ROWS, width), BF),
            jax.ShapeDtypeStruct((LOCAL, ROWS, 2 * width), BF),
            jax.ShapeDtypeStruct((LOCAL, ROWS, D), BF), jax.ShapeDtypeStruct((LOCAL, ROWS, D), BF),
            jax.ShapeDtypeStruct((TP - 1, per) + w_down.shape[1:], BF), jax.ShapeDtypeStruct((NDEV, 2 * TOK, D), BF),
            jax.ShapeDtypeStruct((TP - 1, per, ROWS, width), BF)],
        compiler_params=pltpu.CompilerParams(collective_id=0, has_side_effects=True, vmem_limit_bytes=58 << 20),
        cost_estimate=pl.CostEstimate(flops=60_000_000_000, bytes_accessed=60_000_000, transcendentals=4_000_000),
    )(x, grad_y, table, w_down, w_router, ws_gate, ws_up, ws_down, perm, w_gate, w_up, w_down)


def grad_kernel(xe_ref, de_ref, h_ref, dab_ref, dg_ref, du_ref, dd_ref):
    both = dot_tn(xe_ref[0], dab_ref[0])
    width = both.shape[1] // 2
    dg_ref[0] = both[:, :width]
    du_ref[0] = both[:, width:]
    dd_ref[0] = dot_tn(h_ref[0], de_ref[0])


def grad_call(xe, de, h, dab):
    width = h.shape[2]

    def one(shape):
        return pl.BlockSpec((1,) + shape, lambda i: (i, 0, 0))

    return pl.pallas_call(
        grad_kernel,
        name='grad_call',
        grid=(LOCAL,),
        in_specs=[one((ROWS, D)), one((ROWS, D)), one((ROWS, width)), one((ROWS, 2 * width))],
        out_specs=[one((D, width)), one((D, width)), one((width, D))],
        out_shape=[jax.ShapeDtypeStruct((LOCAL, D, width), F32), jax.ShapeDtypeStruct((LOCAL, D, width), F32),
                   jax.ShapeDtypeStruct((LOCAL, width, D), F32)],
        compiler_params=pltpu.CompilerParams(vmem_limit_bytes=40 << 20),
        cost_estimate=pl.CostEstimate(flops=10_000_000_000, bytes_accessed=55_000_000, transcendentals=0),
    )(xe, de, h, dab)


def out_kernel(tp_ref, h0, h1, h2, h3, w0, w1, w2, w3, o_ref):
    total = dot(jnp.concatenate([h0[0], h1[0, 0], h2[0, 0], h3[0, 0]], axis=1), jnp.concatenate([w0[0], w1[0, 0], w2[0, 0], w3[0, 0]], axis=0))
    for e in range(LOCAL // TP):
        @pl.when(pl.program_id(0) == e)
        def _(e=e):
            for j in range(TP):
                for s in range(EP):
                    first = STRIP * (j * EP + s)
                    o_ref[s * TP + j, STRIP * e:STRIP * (e + 1), :] = total[first:first + STRIP].astype(BF)


def out_call(tp, h, h_in, w, w_in):
    width = h.shape[2]
    per = LOCAL // TP

    def own(shape):
        return pl.BlockSpec((1,) + shape, lambda i, t: (t[0] * per + i, 0, 0))

    def got(shape):
        return [pl.BlockSpec((1, 1) + shape, lambda i, t, m=m: (m, i, 0, 0)) for m in range(TP - 1)]

    return pl.pallas_call(
        out_kernel,
        name='out_call',
        grid_spec=pltpu.PrefetchScalarGridSpec(
            num_scalar_prefetch=1,
            grid=(per,),
            in_specs=[own((ROWS, width))] + got((ROWS, width)) + [own((width, D))] + got((width, D)),
            out_specs=pl.BlockSpec((NDEV, per * STRIP, D), lambda i, t: (0, 0, 0)),
        ),
        out_shape=jax.ShapeDtypeStruct((NDEV, per * STRIP, D), BF),
        compiler_params=pltpu.CompilerParams(vmem_limit_bytes=40 << 20),
        cost_estimate=pl.CostEstimate(flops=5_000_000_000, bytes_accessed=10_000_000, transcendentals=0),
    )(tp, h, h_in, h_in, h_in, w, w_in, w_in, w_in)


def finish_kernel(keep0, keep1, first0, first1, o_ref, x_ref, gy_ref, wr_ref, mark_ref, mark16_ref, all_hbm,
                  y_ref, dx_ref, drt_ref,
                  k1, f1, k0, f0, snd, rcv, ret, ret_in, o_in, dl, xa, s_rows, d_rows,
                  load_sem, x_sem, s2_send, s2_recv, ret_send, ret_recv, o_send, o_recv, dl_send, dl_recv, local_sem):
    tp = lax.axis_index('tp')
    ep = lax.axis_index('ep')
    me = ep * TP + tp

    def peer(mask):
        return (flip_mask(tp, mask & 3), flip_mask(ep, mask >> 2))

    pieces = [(c, i) for i in range(PER_CHUNK) for c in range(CHUNKS)]
    loads = []
    for n, (c, i) in enumerate(pieces):
        rows = pl.ds(BLK * i, BLK)
        keep, first = (keep0, keep1)[c], (first0, first1)[c]
        loads.append([pltpu.make_async_copy(src, dst.at[n], load_sem.at[m, n]) for m, (src, dst) in enumerate((
            (keep.at[1, rows], k1), (first.at[1, rows], f1), (keep.at[0, rows], k0), (first.at[0, rows], f0)))])
    for group in (slice(0, 2), slice(2, 4)):
        for load in loads:
            for copy in load[group]:
                copy.start()
    x_load = pltpu.make_async_copy(all_hbm.at[:, pl.ds(0, TOK), :], xa, x_sem)
    x_load.start()

    barrier = pltpu.get_barrier_semaphore()
    for mask in range(1, NDEV):
        pl.semaphore_signal(barrier, inc=1, device_id=peer(mask), device_id_type=MESH)
    pl.semaphore_wait(barrier, NDEV - 1)

    sent = []

    def send(src, dst, sems, at, mask):
        copy = pltpu.make_async_remote_copy(src_ref=src, dst_ref=dst, send_sem=sems[0].at[at], recv_sem=sems[1].at[at],
                                            device_id=peer(mask), device_id_type=MESH)
        copy.start()
        sent.append(copy)

    def arrived(dst, sems, at):
        pltpu.make_async_remote_copy(src_ref=dst, dst_ref=dst, send_sem=sems[0].at[at], recv_sem=sems[1].at[at],
                                     device_id=peer(BIT_C), device_id_type=MESH).wait_recv()

    for mask in range(1, NDEV):
        send(o_ref.at[flip_mask(me, mask)], o_in.at[me], (o_send, o_recv), mask, mask)
    o_own = pltpu.make_async_copy(o_ref.at[me], o_in.at[me], local_sem)
    o_own.start()

    def second_stage(n):
        loads[n][0].wait()
        loads[n][1].wait()
        snd[n] = k1[n] + f1[n]
        send(snd.at[n], rcv.at[n], (s2_send, s2_recv), n, (BIT_Y, BIT_Z)[pieces[n][0]])

    for n in range(4):
        second_stage(n)

    x = x_ref[...]
    wr = wr_ref[...]
    logits = dot_nt(x, wr)
    ex = jnp.exp(logits - jnp.max(logits, axis=-1, keepdims=True))
    probs = ex / jnp.sum(ex, axis=-1, keepdims=True)
    slots = EXPERTS * STRIP
    spread = (lax.broadcasted_iota(jnp.int32, (EXPERTS, slots), 1) // STRIP == lax.broadcasted_iota(jnp.int32, (EXPERTS, slots), 0))
    spread = jnp.where(spread, 1.0, 0.0).astype(BF)
    mark = mark_ref[...]
    hi, mid, low = split3(GATE_SCALE * probs)
    gate = (dot(hi, spread) + dot(mid, spread) + dot(low, spread)) * mark
    for mask in range(1, NDEV):
        arrived(o_in.at[flip_mask(me, mask)], (o_send, o_recv), mask)
    o_own.wait()
    o_rows = o_in[...].reshape(slots, D)
    hi, mid, low = split3(gate)
    routed = dot(hi, o_rows) + dot(mid, o_rows) + dot(low, o_rows)
    seen = dot_nt(gy_ref[...], o_rows) * mark
    hi, mid, low = split3(seen)
    d_scores = GATE_SCALE * (dot_nt(hi, spread) + dot_nt(mid, spread) + dot_nt(low, spread))
    d_logits = probs * (d_scores - jnp.sum(probs * d_scores, axis=-1, keepdims=True))
    dl[me] = jnp.concatenate([d_logits[:TOK // 2], d_logits[TOK // 2:]], axis=1)
    for mask in range(1, NDEV):
        send(dl.at[me], dl.at[me], (dl_send, dl_recv), mask, mask)
    for n in range(4, len(pieces)):
        second_stage(n)
    hi, mid, low = split3(d_logits)
    dx_router = dot(hi, wr) + dot(mid, wr) + dot(low, wr)

    def finish_piece(n):
        c, i = pieces[n]
        arrived(rcv.at[n], (s2_send, s2_recv), n)
        loads[n][2].wait()
        loads[n][3].wait()
        own = k0[n] + f0[n] + rcv[n]
        for s in range(EP):
            rows = own[2 * CAP * s:2 * CAP * (s + 1)]
            ret[s, n] = jnp.concatenate([rows, jnp.zeros((16 - 2 * CAP, D), F32)], axis=0).astype(BF)
        for at, mask in enumerate((BIT_X, BIT_C, BIT_X | BIT_C)):
            send(ret.at[flip_mask(ep, mask >> 2), n], ret_in.at[ep, n], (ret_send, ret_recv), (n, at), mask)
        ret_in[ep, n] = ret[ep, n]
        (s_rows, d_rows)[c][SH_ROWS * i:SH_ROWS * (i + 1), :] = own[PAIR_ROWS:]

    for n in range(4):
        finish_piece(n)
    for mask in range(1, NDEV):
        arrived(dl.at[flip_mask(me, mask)], (dl_send, dl_recv), mask)
    x_load.wait()
    total = jnp.zeros((EXPERTS, D), F32)
    for half in range(2):
        x_half = xa[:, TOK // 2 * half:TOK // 2 * (half + 1), :].reshape(NDEV * TOK // 2, D)
        for part in split3(dl[...].reshape(NDEV * TOK // 2, 2 * EXPERTS)):
            total = total + dot_tn(part, x_half)[EXPERTS * half:EXPERTS * (half + 1)]
    drt_ref[...] = total
    for n in range(4, len(pieces)):
        finish_piece(n)
    y_ref[...] = (s_rows[...] + routed).astype(BF)
    for n in range(len(pieces)):
        for at, mask in enumerate((BIT_X, BIT_C, BIT_X | BIT_C)):
            arrived(ret_in.at[flip_mask(ep, mask >> 2), n], (ret_send, ret_recv), (n, at))
    back = ret_in[...].reshape(EP * STEPS * 16, D)
    dx_ref[...] = (dx_router + d_rows[...] + dot(mark16_ref[...], back)).astype(BF)
    for copy in sent:
        copy.wait_send()


def finish_call(keeps, firsts, o_send, x, grad_y, w_router, mark, mark16, all_rows):
    vmem = pl.BlockSpec(memory_space=pltpu.VMEM)
    anys = pl.BlockSpec(memory_space=pl.ANY)
    pieces = PER_CHUNK * CHUNKS
    piece = pltpu.VMEM((pieces, BLK, D), F32)
    ret = pltpu.VMEM((EP, pieces, 16, D), BF)
    dma = pltpu.SemaphoreType.DMA
    return pl.pallas_call(
        finish_kernel,
        name='finish_call',
        out_shape=(jax.ShapeDtypeStruct((TOK, D), BF), jax.ShapeDtypeStruct((TOK, D), BF), jax.ShapeDtypeStruct((EXPERTS, D), F32)),
        in_specs=[anys] * 4 + [vmem] * 6 + [anys],
        out_specs=(vmem, vmem, vmem),
        scratch_shapes=[piece] * 6 + [ret, ret, pltpu.VMEM((NDEV, LOCAL // TP * STRIP, D), BF), pltpu.VMEM((NDEV, TOK // 2, 2 * EXPERTS), F32),
                                      pltpu.VMEM((NDEV, TOK, D), BF), pltpu.VMEM((TOK, D), F32), pltpu.VMEM((TOK, D), F32),
                                      dma((4, pieces)), dma, dma((pieces,)), dma((pieces,)), dma((pieces, 3)), dma((pieces, 3)),
                                      dma((NDEV,)), dma((NDEV,)), dma((NDEV,)), dma((NDEV,)), dma],
        compiler_params=pltpu.CompilerParams(collective_id=1, has_side_effects=True, vmem_limit_bytes=48 << 20),
        cost_estimate=pl.CostEstimate(flops=50_000_000_000, bytes_accessed=20_000_000, transcendentals=0),
    )(*keeps, *firsts, o_send, x, grad_y, w_router, mark, mark16, all_rows)


def permutations():
    row = np.arange(TP * PAIR_ROWS)
    col, rest = row // PAIR_ROWS, row % PAIR_ROWS
    src, rest = rest // (2 * CAP), rest % (2 * CAP)
    which, slot = rest // CAP, rest % CAP
    hit = (col * (EP * STRIP) + src * STRIP + slot)[:, None] == np.arange(ROWS)[None, :]
    return jnp.asarray(np.stack([hit & (which == i)[:, None] for i in range(2)]), dtype=BF)


def solution(mesh):
    def device_body(x, grad_y, w_router, w_gate, w_up, w_down, ws_gate, ws_up, ws_down, topk_idx):
        tp = lax.axis_index('tp')
        ids = jnp.arange(EXPERTS, dtype=jnp.int32)
        hit = jnp.any(topk_idx[:, :, None] == ids[None, None, :], axis=1)
        before = jnp.tril(jnp.ones((TOK, TOK), BF), -1)
        rank = dot(before, hit.astype(BF))
        rank = jnp.where(hit, rank, -1.0).astype(jnp.int32)
        slot_hit = rank[:, :, None] == jnp.arange(STRIP, dtype=jnp.int32)[None, None, :]
        *parts, h, dab, xe, de, w_in, all_rows, h_in = main_call(
            x, grad_y, topk_idx.T, w_router.T, ws_gate, ws_up, ws_down, permutations(), w_gate, w_up, w_down)
        firsts = [lax.ppermute(parts[2 * c + 1], 'tp', [(s, s ^ (2 - c)) for s in range(TP)]) for c in range(CHUNKS)]
        o_send = out_call(tp.reshape(1), h, h_in, w_down, w_in)

        d_w_gate, d_w_up, d_w_down = grad_call(xe, de, h, dab)

        x_all = all_rows[:, :TOK].reshape(NDEV * TOK, D)
        gy_all = all_rows[:, TOK:].reshape(NDEV * TOK, D)
        sa = dot(x_all, ws_gate).astype(BF).astype(F32)
        sb = dot(x_all, ws_up).astype(BF).astype(F32)
        sdh = dot_nt(gy_all, ws_down).astype(BF).astype(F32)
        s_h, s_da, s_db = act_both(sa, sb, sdh)
        ds_gate = dot_tn(x_all, s_da)
        ds_up = dot_tn(x_all, s_db)
        ds_down = dot_tn(s_h, gy_all)

        mark = slot_hit.reshape(TOK, EXPERTS * STRIP).astype(F32)
        mark16 = slot_hit[:, :, :CAP].reshape(TOK, EP, CHUNKS, PER_CHUNK, 2 * CAP).transpose(0, 1, 3, 2, 4)
        mark16 = jnp.pad(mark16, ((0, 0),) * 4 + ((0, 16 - 2 * CAP),)).reshape(TOK, EP * STEPS * 16).astype(BF)
        y_out, dx_out, d_router = finish_call(parts[0::2], firsts, o_send, x, grad_y, w_router.T, mark, mark16, all_rows)
        d_router = d_router.T
        return y_out, dx_out, d_router, d_w_gate, d_w_up, d_w_down, ds_gate, ds_up, ds_down

    tok_spec = P(('ep', 'tp'), None)
    in_specs = (tok_spec, tok_spec, P(None, None), P('ep', None, 'tp'), P('ep', None, 'tp'), P('ep', 'tp', None), P(None, 'tp'), P(None, 'tp'), P('tp', None), tok_spec)
    out_specs = (tok_spec, tok_spec, P(None, None), P('ep', None, 'tp'), P('ep', None, 'tp'), P('ep', 'tp', None), P(None, 'tp'), P(None, 'tp'), P('tp', None))
    return jax.shard_map(device_body, mesh=mesh, in_specs=in_specs, out_specs=out_specs, check_vma=False)
```

```python
import jax
import jax.numpy as jnp
import numpy as np
from jax import lax
from jax.experimental import pallas as pl
from jax.experimental.pallas import tpu as pltpu
from jax.sharding import PartitionSpec as P


GATE_SCALE = 16.0
BF = jnp.bfloat16
F32 = jnp.float32
MESH = pl.DeviceIdType.MESH

D = 1536
EXPERTS = 64
TOP = 6
TOK = 64
TP = 4
EP = 4
NDEV = TP * EP
LOCAL = EXPERTS // EP
CAP = 7
STRIP = 8
ROWS = NDEV * STRIP
PAIR_ROWS = 2 * EP * CAP
STEPS = LOCAL // 2
SH_ROWS = 2 * TOK // STEPS
BLK = PAIR_ROWS + SH_ROWS
CHUNKS = 2
PER_CHUNK = STEPS // CHUNKS
PARTS = 4

BIT_Y, BIT_Z, BIT_C, BIT_X = 1, 2, 4, 8


def flip(value, bit):
    return value + bit * (1 - 2 * ((value // bit) % 2))


def flip_mask(value, mask):
    for bit in (1, 2, 4, 8):
        if mask & bit:
            value = flip(value, bit)
    return value


def dot(a, b):
    return jnp.dot(a, b, preferred_element_type=F32)


def dot_nt(a, b):
    return lax.dot_general(a, b, (((1,), (1,)), ((), ())), preferred_element_type=F32)


def dot_tn(a, b):
    return lax.dot_general(a, b, (((0,), (0,)), ((), ())), preferred_element_type=F32)


def act_both(a, b, dh):
    sig = 1.0 / (1.0 + jnp.exp(-a))
    silu = a * sig
    h = (silu * b).astype(BF)
    db = (dh * silu).astype(BF)
    da = (dh * b * (sig * (1.0 + a * (1.0 - sig)))).astype(BF)
    return h, da, db


def gather_rows(x_ref, gy_ref, tab_ref, w_ref, all_ref, tabs_ref, w_in_ref, keep_ref, send_sem, recv_sem, local_sem, w_send, w_recv, keep_sem):
    tp = lax.axis_index('tp')
    ep = lax.axis_index('ep')
    me = ep * TP + tp
    width = D // PARTS

    def peer(mask):
        return (flip_mask(tp, mask & 3), flip_mask(ep, mask >> 2))

    own = [pltpu.make_async_copy(x_ref, all_ref.at[me, pl.ds(0, TOK)], local_sem.at[0]),
           pltpu.make_async_copy(gy_ref, all_ref.at[me, pl.ds(TOK, TOK)], local_sem.at[1]),
           pltpu.make_async_copy(tab_ref, tabs_ref.at[me], local_sem.at[2])]
    for c in own:
        c.start()
    barrier = pltpu.get_barrier_semaphore()
    for mask in (BIT_X, BIT_Y, BIT_Z, BIT_C, BIT_Y | BIT_Z):
        pl.semaphore_signal(barrier, inc=1, device_id=peer(mask), device_id_type=MESH)
    pl.semaphore_wait(barrier, 5)
    for c in own:
        c.wait()

    orders = [(BIT_Y, BIT_Z, BIT_X) if part % 2 == 0 else (BIT_Z, BIT_Y, BIT_X) for part in range(PARTS + 1)]

    def view(part, block):
        if part == PARTS:
            return tabs_ref.at[block]
        return all_ref.at[block, :, pl.ds(part * width, width)]

    sent = []

    def send(part, k, mask):
        block = flip_mask(me, k)
        c = pltpu.make_async_remote_copy(
            src_ref=view(part, block), dst_ref=view(part, block),
            send_sem=send_sem.at[part, k ^ mask], recv_sem=recv_sem.at[part, k ^ mask],
            device_id=peer(mask), device_id_type=MESH)
        c.start()
        sent.append(c)

    def arrived(part, k):
        block = flip_mask(me, k)
        pltpu.make_async_remote_copy(
            src_ref=view(part, block), dst_ref=view(part, block),
            send_sem=send_sem.at[part, k], recv_sem=recv_sem.at[part, k],
            device_id=peer(BIT_C), device_id_type=MESH).wait_recv()

    parts = (PARTS,) + tuple(range(PARTS))
    for step in range(3):
        for part in parts:
            send(part, 0, orders[part][step])
    for part in parts:
        send(part, 0, BIT_C)
    for part in parts:
        m1, m2, m3 = orders[part]
        arrived(part, m1)
        send(part, m1, m2)
        send(part, m1, m3)
        send(part, m1, BIT_C)
    per = LOCAL // TP
    for m in range(1, TP):
        c = pltpu.make_async_remote_copy(src_ref=w_ref.at[pl.ds(flip_mask(tp, m) * per, per)], dst_ref=w_in_ref.at[m - 1],
                                         send_sem=w_send.at[m - 1], recv_sem=w_recv.at[m - 1], device_id=peer(m), device_id_type=MESH)
        c.start()
    for part in parts:
        m1, m2, m3 = orders[part]
        arrived(part, m2)
        send(part, m2, m3)
        send(part, m2, BIT_C)
    for part in parts:
        m1, m2, m3 = orders[part]
        arrived(part, m1 ^ m2)
        send(part, m1 ^ m2, m3)
        send(part, m1 ^ m2, BIT_C)
    for extra in range(4):
        for part in parts:
            m1, m2, m3 = orders[part]
            k = (m3, m1 ^ m3, m2 ^ m3, m1 ^ m2 ^ m3)[extra]
            arrived(part, k)
            send(part, k, BIT_C)
    kept = []
    for k in sorted(range(16), key=lambda k: k & BIT_C):
        if k & BIT_C:
            for part in parts:
                arrived(part, k)
        block = flip_mask(me, k)
        c = pltpu.make_async_copy(all_ref.at[block], keep_ref.at[block], keep_sem.at[k])
        c.start()
        kept.append(c)
    for c in kept:
        c.wait()
    for c in sent:
        c.wait_send()


def split3(v):
    hi = v.astype(BF)
    rest = v - hi.astype(F32)
    mid = rest.astype(BF)
    return hi, mid, (rest - mid.astype(F32)).astype(BF)


def chunk_members(chunk):
    return ((0, 1), (2, 3)) if chunk % 2 == 0 else ((0, 2), (1, 3))


def main_kernel(x_ref, gy_ref, tab_ref, w_all_ref, wr_hbm, wsg_hbm, wsu_hbm, wsd_hbm, perm_ref, wg_ref, wu_ref, wd_ref, *refs):
    chunk_refs, refs = refs[:2 * CHUNKS], refs[2 * CHUNKS:]
    (h_ref, dab_ref, xe_hbm, de_hbm, w_in_ref, keep_ref, h_in_ref, all_ref, tabs_ref, xe, de, sh, hs, sems,
     send_sem, recv_sem, local_sem, w_send, w_recv, keep_sem, h_send, h_recv, wr_ref, wsg_ref, wsu_ref, wsd_ref, late_sem) = refs
    step = pl.program_id(0)
    g = lax.axis_index('ep')
    tp = lax.axis_index('tp')
    third = D // 3
    per = LOCAL // TP
    xe_copy = pltpu.make_async_copy(xe, xe_hbm, sems.at[0])
    de_copy = pltpu.make_async_copy(de, de_hbm, sems.at[1])

    @pl.when(step == 0)
    def _():
        late_copies = [pltpu.make_async_copy(src, dst, late_sem.at[n]) for n, (src, dst) in enumerate((
            (wr_hbm, wr_ref), (wsg_hbm, wsg_ref), (wsu_hbm, wsu_ref), (wsd_hbm, wsd_ref)))]
        for c in late_copies:
            c.start()
        gather_rows(x_ref, gy_ref, tab_ref, w_all_ref, all_ref, tabs_ref, w_in_ref, keep_ref, send_sem, recv_sem, local_sem, w_send, w_recv, keep_sem)
        for c in late_copies:
            c.wait()
        n_rows = LOCAL * EP * STRIP
        expert = g * LOCAL + lax.broadcasted_iota(jnp.int32, (LOCAL, TOK), 0)
        early = lax.broadcasted_iota(jnp.int32, (EP * TOK, EP * TOK), 0)
        late = lax.broadcasted_iota(jnp.int32, (EP * TOK, EP * TOK), 1)
        before = jnp.where((early < late) & (early // TOK == late // TOK), 1.0, 0.0).astype(BF)
        cube = (LOCAL, EP * STRIP, EP * TOK)
        place = lax.broadcasted_iota(jnp.int32, cube, 1)
        wanted_rank = (place % STRIP).astype(F32)
        same_source = place // STRIP == lax.broadcasted_iota(jnp.int32, cube, 2) // TOK
        wr = wr_ref[...]
        row_expert = g * LOCAL + lax.broadcasted_iota(jnp.int32, (n_rows, 3 * EXPERTS), 0) // (EP * STRIP)
        wanted = lax.broadcasted_iota(jnp.int32, (n_rows, 3 * EXPERTS), 1) % EXPERTS == row_expert
        for j in range(TP):
            hit = []
            for s in range(EP):
                ids = tabs_ref[s * TP + j]
                found = ids[0:1, :] == expert
                for k in range(1, TOP):
                    found = found | (ids[k:k + 1, :] == expert)
                hit.append(jnp.where(found, 1.0, 0.0))
            hit = jnp.concatenate(hit, axis=1)
            rank = jnp.where(hit > 0.0, dot(hit.astype(BF), before), -1.0)
            rank = jnp.broadcast_to(rank[:, None, :], cube)
            pick = jnp.where((rank == wanted_rank) & same_source, 1.0, 0.0).reshape(n_rows, EP * TOK).astype(BF)
            x_j = jnp.concatenate([all_ref[s * TP + j, :TOK, :] for s in range(EP)], axis=0)
            logits = dot_nt(x_j, wr)
            top = jnp.max(logits, axis=-1, keepdims=True)
            ex = jnp.exp(logits - top)
            probs = ex / jnp.sum(ex, axis=-1, keepdims=True)
            sel = dot(pick, jnp.concatenate(split3(probs), axis=1))
            gate = GATE_SCALE * jnp.sum(jnp.where(wanted, sel, 0.0), axis=1, keepdims=True)
            for n in range(3):
                cols = slice(n * third, (n + 1) * third)
                got = dot(pick, x_j[:, cols]).astype(BF)
                xe[:, EP * STRIP * j:EP * STRIP * (j + 1), cols] = got.reshape(LOCAL, EP * STRIP, third)
                gy_j = jnp.concatenate([all_ref[s * TP + j, TOK:, cols] for s in range(EP)], axis=0)
                got = (dot(pick, gy_j) * gate).astype(BF)
                de[:, EP * STRIP * j:EP * STRIP * (j + 1), cols] = got.reshape(LOCAL, EP * STRIP, third)
        xe_copy.start()
        de_copy.start()
        x_s = jnp.concatenate([all_ref[g * TP + j, :TOK, :] for j in range(TP)], axis=0)
        gy_s = jnp.concatenate([all_ref[g * TP + j, TOK:, :] for j in range(TP)], axis=0)
        a = dot(x_s, wsg_ref[...]).astype(BF).astype(F32)
        b = dot(x_s, wsu_ref[...]).astype(BF).astype(F32)
        dh = dot_nt(gy_s, wsd_ref[...]).astype(BF).astype(F32)
        h, da, db = act_both(a, b, dh)
        for n in range(3):
            cols = slice(n * third, (n + 1) * third)
            sh[0, :, :, cols] = dot(h, wsd_ref[:, cols]).reshape(TP, TOK, third)
            dxs = dot_nt(da, wsg_ref[cols, :]) + dot_nt(db, wsu_ref[cols, :])
            sh[1, :, :, cols] = dxs.reshape(TP, TOK, third)

    lhs = []
    for i in range(2):
        e = 2 * step + i
        x_e = xe[e]
        ab = dot(x_e, jnp.concatenate([wg_ref[i], wu_ref[i]], axis=1)).astype(BF).astype(F32)
        dh = dot_nt(de[e], wd_ref[i]).astype(BF).astype(F32)
        width = ab.shape[1] // 2
        h, da, db = act_both(ab[:, :width], ab[:, width:], dh)
        h_ref[i] = h
        hs[e] = h
        dab = jnp.concatenate([da, db], axis=1)
        dab_ref[i] = dab
        dab = jnp.concatenate([dab_ref[i, pl.ds(pl.multiple_of(flip_mask(tp, rel) * EP * STRIP, EP * STRIP), EP * STRIP), :] for rel in range(TP)], axis=0)
        lhs.append(dot(perm_ref[i], dab).astype(BF))
    lhs = jnp.concatenate(lhs, axis=1)
    half = step // (STEPS // 2)
    first = pl.multiple_of((step % (STEPS // 2)) * SH_ROWS, SH_ROWS)
    found = []
    for n in range(3):
        cols = slice(n * third, (n + 1) * third)
        rhs = jnp.concatenate([wg_ref[0, cols, :], wu_ref[0, cols, :], wg_ref[1, cols, :], wu_ref[1, cols, :]], axis=1)
        found.append(dot_nt(lhs, rhs).reshape(TP, PAIR_ROWS, third))
    for chunk in range(CHUNKS):
        @pl.when(step // (STEPS // CHUNKS) == chunk)
        def _(chunk=chunk):
            for ref, members in zip(chunk_refs[2 * chunk:2 * chunk + 2], chunk_members(chunk)):
                for at, rel in enumerate(members):
                    for n in range(3):
                        ref[at, :PAIR_ROWS, n * third:(n + 1) * third] = found[n][rel]
                    away = flip_mask(tp, rel)
                    ref[at, PAIR_ROWS:, :] = sh[half, away, pl.ds(first, SH_ROWS), :]

    @pl.when(step == STEPS - 1)
    def _():
        h_copies = []
        for m in range(1, TP):
            to = flip_mask(tp, m)
            c = pltpu.make_async_remote_copy(src_ref=hs.at[pl.ds(to * per, per)], dst_ref=h_in_ref.at[m - 1],
                                             send_sem=h_send.at[m - 1], recv_sem=h_recv.at[m - 1], device_id=(to, g), device_id_type=MESH)
            c.start()
            h_copies.append(c)
        xe_copy.wait()
        de_copy.wait()
        for m in range(1, TP):
            to = flip_mask(tp, m)
            pltpu.make_async_remote_copy(src_ref=w_all_ref.at[pl.ds(to * per, per)], dst_ref=w_in_ref.at[m - 1],
                                         send_sem=w_send.at[m - 1], recv_sem=w_recv.at[m - 1], device_id=(to, g), device_id_type=MESH).wait()
        for c in h_copies:
            c.wait()


def main_call(x, grad_y, table, w_router, ws_gate, ws_up, ws_down, perm, w_gate, w_up, w_down):
    width = w_gate.shape[2]
    per = LOCAL // TP

    def whole(a):
        return pl.BlockSpec(a.shape, lambda i: (0,) * a.ndim, pipeline_mode=pl.Buffered(1))

    def pair(a):
        return pl.BlockSpec((2,) + a.shape[1:], lambda i: (i, 0, 0))

    hbm = pl.BlockSpec(memory_space=pltpu.HBM)
    dma = pltpu.SemaphoreType.DMA
    chunk_specs = [pl.BlockSpec((2, BLK, D), lambda i, c=n // 2: (0, jnp.clip(i - PER_CHUNK * c, 0, PER_CHUNK - 1), 0))
                   for n in range(2 * CHUNKS)]
    return pl.pallas_call(
        main_kernel,
        name='main_call',
        grid=(STEPS,),
        in_specs=[hbm] * 8 + [whole(perm),
                  pair(w_gate), pair(w_up), pair(w_down)],
        out_specs=chunk_specs + [
            pl.BlockSpec((2, ROWS, width), lambda i: (i, 0, 0)),
            pl.BlockSpec((2, ROWS, 2 * width), lambda i: (i, 0, 0)), hbm, hbm, hbm, hbm, hbm],
        scratch_shapes=[pltpu.VMEM((NDEV, 2 * TOK, D), BF), pltpu.VMEM((NDEV,) + table.shape, jnp.int32),
                        pltpu.VMEM((LOCAL, ROWS, D), BF), pltpu.VMEM((LOCAL, ROWS, D), BF),
                        pltpu.VMEM((2, TP, TOK, D), F32), pltpu.VMEM((LOCAL, ROWS, width), BF), dma((2,)),
                        dma((PARTS + 1, 16)), dma((PARTS + 1, 16)), dma((3,)), dma((TP - 1,)), dma((TP - 1,)), dma((NDEV,)), dma((TP - 1,)), dma((TP - 1,)),
                        pltpu.VMEM(w_router.shape, BF), pltpu.VMEM(ws_gate.shape, BF), pltpu.VMEM(ws_up.shape, BF), pltpu.VMEM(ws_down.shape, BF), dma((4,))],
        out_shape=[jax.ShapeDtypeStruct((2, BLK * PER_CHUNK, D), F32)] * (2 * CHUNKS) + [
            jax.ShapeDtypeStruct((LOCAL, ROWS, width), BF),
            jax.ShapeDtypeStruct((LOCAL, ROWS, 2 * width), BF),
            jax.ShapeDtypeStruct((LOCAL, ROWS, D), BF), jax.ShapeDtypeStruct((LOCAL, ROWS, D), BF),
            jax.ShapeDtypeStruct((TP - 1, per) + w_down.shape[1:], BF), jax.ShapeDtypeStruct((NDEV, 2 * TOK, D), BF),
            jax.ShapeDtypeStruct((TP - 1, per, ROWS, width), BF)],
        compiler_params=pltpu.CompilerParams(collective_id=0, has_side_effects=True, vmem_limit_bytes=58 << 20),
        cost_estimate=pl.CostEstimate(flops=60_000_000_000, bytes_accessed=60_000_000, transcendentals=4_000_000),
    )(x, grad_y, table, w_down, w_router, ws_gate, ws_up, ws_down, perm, w_gate, w_up, w_down)


def grad_kernel(xe_ref, de_ref, h_ref, dab_ref, dg_ref, du_ref, dd_ref):
    both = dot_tn(xe_ref[0], dab_ref[0])
    width = both.shape[1] // 2
    dg_ref[0] = both[:, :width]
    du_ref[0] = both[:, width:]
    dd_ref[0] = dot_tn(h_ref[0], de_ref[0])


def grad_call(xe, de, h, dab):
    width = h.shape[2]

    def one(shape):
        return pl.BlockSpec((1,) + shape, lambda i: (i, 0, 0))

    return pl.pallas_call(
        grad_kernel,
        name='grad_call',
        grid=(LOCAL,),
        in_specs=[one((ROWS, D)), one((ROWS, D)), one((ROWS, width)), one((ROWS, 2 * width))],
        out_specs=[one((D, width)), one((D, width)), one((width, D))],
        out_shape=[jax.ShapeDtypeStruct((LOCAL, D, width), F32), jax.ShapeDtypeStruct((LOCAL, D, width), F32),
                   jax.ShapeDtypeStruct((LOCAL, width, D), F32)],
        compiler_params=pltpu.CompilerParams(vmem_limit_bytes=40 << 20),
        cost_estimate=pl.CostEstimate(flops=10_000_000_000, bytes_accessed=55_000_000, transcendentals=0),
    )(xe, de, h, dab)


def out_kernel(tp_ref, h0, h1, h2, h3, w0, w1, w2, w3, o_ref):
    total = dot(jnp.concatenate([h0[0], h1[0, 0], h2[0, 0], h3[0, 0]], axis=1), jnp.concatenate([w0[0], w1[0, 0], w2[0, 0], w3[0, 0]], axis=0))
    for e in range(LOCAL // TP):
        @pl.when(pl.program_id(0) == e)
        def _(e=e):
            for j in range(TP):
                for s in range(EP):
                    first = STRIP * (j * EP + s)
                    o_ref[s * TP + j, STRIP * e:STRIP * (e + 1), :] = total[first:first + STRIP].astype(BF)


def out_call(tp, h, h_in, w, w_in):
    width = h.shape[2]
    per = LOCAL // TP

    def own(shape):
        return pl.BlockSpec((1,) + shape, lambda i, t: (t[0] * per + i, 0, 0))

    def got(shape):
        return [pl.BlockSpec((1, 1) + shape, lambda i, t, m=m: (m, i, 0, 0)) for m in range(TP - 1)]

    return pl.pallas_call(
        out_kernel,
        name='out_call',
        grid_spec=pltpu.PrefetchScalarGridSpec(
            num_scalar_prefetch=1,
            grid=(per,),
            in_specs=[own((ROWS, width))] + got((ROWS, width)) + [own((width, D))] + got((width, D)),
            out_specs=pl.BlockSpec((NDEV, per * STRIP, D), lambda i, t: (0, 0, 0)),
        ),
        out_shape=jax.ShapeDtypeStruct((NDEV, per * STRIP, D), BF),
        compiler_params=pltpu.CompilerParams(vmem_limit_bytes=40 << 20),
        cost_estimate=pl.CostEstimate(flops=5_000_000_000, bytes_accessed=10_000_000, transcendentals=0),
    )(tp, h, h_in, h_in, h_in, w, w_in, w_in, w_in)


def finish_kernel(keep0, keep1, first0, first1, o_ref, x_ref, gy_ref, wr_ref, mark_ref, mark16_ref, all_hbm,
                  y_ref, dx_ref, drt_ref,
                  k1, f1, k0, f0, snd, rcv, ret, ret_in, o_in, dl, xa, s_rows, d_rows,
                  load_sem, x_sem, s2_send, s2_recv, ret_send, ret_recv, o_send, o_recv, dl_send, dl_recv, local_sem):
    tp = lax.axis_index('tp')
    ep = lax.axis_index('ep')
    me = ep * TP + tp

    def peer(mask):
        return (flip_mask(tp, mask & 3), flip_mask(ep, mask >> 2))

    pieces = [(c, i) for i in range(PER_CHUNK) for c in range(CHUNKS)]
    loads = []
    for n, (c, i) in enumerate(pieces):
        rows = pl.ds(BLK * i, BLK)
        keep, first = (keep0, keep1)[c], (first0, first1)[c]
        loads.append([pltpu.make_async_copy(src, dst.at[n], load_sem.at[m, n]) for m, (src, dst) in enumerate((
            (keep.at[1, rows], k1), (first.at[1, rows], f1), (keep.at[0, rows], k0), (first.at[0, rows], f0)))])
    for group in (slice(0, 2), slice(2, 4)):
        for load in loads:
            for copy in load[group]:
                copy.start()
    x_load = pltpu.make_async_copy(all_hbm.at[:, pl.ds(0, TOK), :], xa, x_sem)
    x_load.start()

    barrier = pltpu.get_barrier_semaphore()
    for mask in range(1, NDEV):
        pl.semaphore_signal(barrier, inc=1, device_id=peer(mask), device_id_type=MESH)
    pl.semaphore_wait(barrier, NDEV - 1)

    sent = []

    def send(src, dst, sems, at, mask):
        copy = pltpu.make_async_remote_copy(src_ref=src, dst_ref=dst, send_sem=sems[0].at[at], recv_sem=sems[1].at[at],
                                            device_id=peer(mask), device_id_type=MESH)
        copy.start()
        sent.append(copy)

    def arrived(dst, sems, at):
        pltpu.make_async_remote_copy(src_ref=dst, dst_ref=dst, send_sem=sems[0].at[at], recv_sem=sems[1].at[at],
                                     device_id=peer(BIT_C), device_id_type=MESH).wait_recv()

    for mask in range(1, NDEV):
        send(o_ref.at[flip_mask(me, mask)], o_in.at[me], (o_send, o_recv), mask, mask)
    o_own = pltpu.make_async_copy(o_ref.at[me], o_in.at[me], local_sem)
    o_own.start()

    def second_stage(n):
        loads[n][0].wait()
        loads[n][1].wait()
        snd[n] = k1[n] + f1[n]
        pass_rows(n, 0)

    def pass_rows(n, which):
        rows = (pl.ds(0, PAIR_ROWS), pl.ds(PAIR_ROWS, SH_ROWS))[which]
        send(snd.at[n, rows], rcv.at[n, rows], (s2_send, s2_recv), (n, which), (BIT_Y, BIT_Z)[pieces[n][0]])

    for n in range(4):
        second_stage(n)

    x = x_ref[...]
    wr = wr_ref[...]
    logits = dot_nt(x, wr)
    ex = jnp.exp(logits - jnp.max(logits, axis=-1, keepdims=True))
    probs = ex / jnp.sum(ex, axis=-1, keepdims=True)
    slots = EXPERTS * STRIP
    spread = (lax.broadcasted_iota(jnp.int32, (EXPERTS, slots), 1) // STRIP == lax.broadcasted_iota(jnp.int32, (EXPERTS, slots), 0))
    spread = jnp.where(spread, 1.0, 0.0).astype(BF)
    mark = mark_ref[...]
    hi, mid, low = split3(GATE_SCALE * probs)
    gate = (dot(hi, spread) + dot(mid, spread) + dot(low, spread)) * mark
    for mask in range(1, NDEV):
        arrived(o_in.at[flip_mask(me, mask)], (o_send, o_recv), mask)
    o_own.wait()
    o_rows = o_in[...].reshape(slots, D)
    hi, mid, low = split3(gate)
    routed = dot(hi, o_rows) + dot(mid, o_rows) + dot(low, o_rows)
    seen = dot_nt(gy_ref[...], o_rows) * mark
    hi, mid, low = split3(seen)
    d_scores = GATE_SCALE * (dot_nt(hi, spread) + dot_nt(mid, spread) + dot_nt(low, spread))
    d_logits = probs * (d_scores - jnp.sum(probs * d_scores, axis=-1, keepdims=True))
    dl[me] = jnp.concatenate([d_logits[:TOK // 2], d_logits[TOK // 2:]], axis=1)
    columns, copies = (BIT_Y, BIT_Z, BIT_Y | BIT_Z), (BIT_X, BIT_C, BIT_X | BIT_C)

    def pass_dl(k, mask):
        block = dl.at[flip_mask(me, k)]
        send(block, block, (dl_send, dl_recv), k ^ mask, mask)

    for mask in columns + copies:
        pass_dl(0, mask)
    for n in range(4, len(pieces)):
        second_stage(n)
    for n in range(len(pieces)):
        pass_rows(n, 1)
    hi, mid, low = split3(d_logits)
    dx_router = dot(hi, wr) + dot(mid, wr) + dot(low, wr)

    def finish_piece(n):
        arrived(rcv.at[n, pl.ds(0, PAIR_ROWS)], (s2_send, s2_recv), (n, 0))
        loads[n][2].wait()
        loads[n][3].wait()
        own = k0[n, :PAIR_ROWS] + f0[n, :PAIR_ROWS] + rcv[n, :PAIR_ROWS]
        for s in range(EP):
            rows = own[2 * CAP * s:2 * CAP * (s + 1)]
            ret[s, n] = jnp.concatenate([rows, jnp.zeros((16 - 2 * CAP, D), F32)], axis=0).astype(BF)
        for at, mask in enumerate((BIT_X, BIT_C, BIT_X | BIT_C)):
            send(ret.at[flip_mask(ep, mask >> 2), n], ret_in.at[ep, n], (ret_send, ret_recv), (n, at), mask)
        ret_in[ep, n] = ret[ep, n]

    for n in range(4):
        finish_piece(n)
    for k in columns:
        arrived(dl.at[flip_mask(me, k)], (dl_send, dl_recv), k)
        for mask in copies:
            pass_dl(k, mask)
    for k in range(TP, NDEV):
        arrived(dl.at[flip_mask(me, k)], (dl_send, dl_recv), k)
    x_load.wait()
    total = jnp.zeros((EXPERTS, D), F32)
    for half in range(2):
        x_half = xa[:, TOK // 2 * half:TOK // 2 * (half + 1), :].reshape(NDEV * TOK // 2, D)
        for part in split3(dl[...].reshape(NDEV * TOK // 2, 2 * EXPERTS)):
            total = total + dot_tn(part, x_half)[EXPERTS * half:EXPERTS * (half + 1)]
    drt_ref[...] = total
    for n in range(4, len(pieces)):
        finish_piece(n)
    for n, (c, i) in enumerate(pieces):
        arrived(rcv.at[n, pl.ds(PAIR_ROWS, SH_ROWS)], (s2_send, s2_recv), (n, 1))
        (s_rows, d_rows)[c][SH_ROWS * i:SH_ROWS * (i + 1), :] = k0[n, PAIR_ROWS:] + f0[n, PAIR_ROWS:] + rcv[n, PAIR_ROWS:]
    y_ref[...] = (s_rows[...] + routed).astype(BF)
    for n in range(len(pieces)):
        for at, mask in enumerate((BIT_X, BIT_C, BIT_X | BIT_C)):
            arrived(ret_in.at[flip_mask(ep, mask >> 2), n], (ret_send, ret_recv), (n, at))
    back = ret_in[...].reshape(EP * STEPS * 16, D)
    dx_ref[...] = (dx_router + d_rows[...] + dot(mark16_ref[...], back)).astype(BF)
    for copy in sent:
        copy.wait_send()


def finish_call(keeps, firsts, o_send, x, grad_y, w_router, mark, mark16, all_rows):
    vmem = pl.BlockSpec(memory_space=pltpu.VMEM)
    anys = pl.BlockSpec(memory_space=pl.ANY)
    pieces = PER_CHUNK * CHUNKS
    piece = pltpu.VMEM((pieces, BLK, D), F32)
    ret = pltpu.VMEM((EP, pieces, 16, D), BF)
    dma = pltpu.SemaphoreType.DMA
    return pl.pallas_call(
        finish_kernel,
        name='finish_call',
        out_shape=(jax.ShapeDtypeStruct((TOK, D), BF), jax.ShapeDtypeStruct((TOK, D), BF), jax.ShapeDtypeStruct((EXPERTS, D), F32)),
        in_specs=[anys] * 4 + [vmem] * 6 + [anys],
        out_specs=(vmem, vmem, vmem),
        scratch_shapes=[piece] * 6 + [ret, ret, pltpu.VMEM((NDEV, LOCAL // TP * STRIP, D), BF), pltpu.VMEM((NDEV, TOK // 2, 2 * EXPERTS), F32),
                                      pltpu.VMEM((NDEV, TOK, D), BF), pltpu.VMEM((TOK, D), F32), pltpu.VMEM((TOK, D), F32),
                                      dma((4, pieces)), dma, dma((pieces, 2)), dma((pieces, 2)), dma((pieces, 3)), dma((pieces, 3)),
                                      dma((NDEV,)), dma((NDEV,)), dma((NDEV,)), dma((NDEV,)), dma],
        compiler_params=pltpu.CompilerParams(collective_id=1, has_side_effects=True, vmem_limit_bytes=48 << 20),
        cost_estimate=pl.CostEstimate(flops=50_000_000_000, bytes_accessed=20_000_000, transcendentals=0),
    )(*keeps, *firsts, o_send, x, grad_y, w_router, mark, mark16, all_rows)


def permutations():
    row = np.arange(TP * PAIR_ROWS)
    col, rest = row // PAIR_ROWS, row % PAIR_ROWS
    src, rest = rest // (2 * CAP), rest % (2 * CAP)
    which, slot = rest // CAP, rest % CAP
    hit = (col * (EP * STRIP) + src * STRIP + slot)[:, None] == np.arange(ROWS)[None, :]
    return jnp.asarray(np.stack([hit & (which == i)[:, None] for i in range(2)]), dtype=BF)


def solution(mesh):
    def device_body(x, grad_y, w_router, w_gate, w_up, w_down, ws_gate, ws_up, ws_down, topk_idx):
        tp = lax.axis_index('tp')
        ids = jnp.arange(EXPERTS, dtype=jnp.int32)
        hit = jnp.any(topk_idx[:, :, None] == ids[None, None, :], axis=1)
        before = jnp.tril(jnp.ones((TOK, TOK), BF), -1)
        rank = dot(before, hit.astype(BF))
        rank = jnp.where(hit, rank, -1.0).astype(jnp.int32)
        slot_hit = rank[:, :, None] == jnp.arange(STRIP, dtype=jnp.int32)[None, None, :]
        *parts, h, dab, xe, de, w_in, all_rows, h_in = main_call(
            x, grad_y, topk_idx.T, w_router.T, ws_gate, ws_up, ws_down, permutations(), w_gate, w_up, w_down)
        firsts = [lax.ppermute(parts[2 * c + 1], 'tp', [(s, s ^ (2 - c)) for s in range(TP)]) for c in range(CHUNKS)]
        o_send = out_call(tp.reshape(1), h, h_in, w_down, w_in)

        d_w_gate, d_w_up, d_w_down = grad_call(xe, de, h, dab)

        x_all = all_rows[:, :TOK].reshape(NDEV * TOK, D)
        gy_all = all_rows[:, TOK:].reshape(NDEV * TOK, D)
        sa = dot(x_all, ws_gate).astype(BF).astype(F32)
        sb = dot(x_all, ws_up).astype(BF).astype(F32)
        sdh = dot_nt(gy_all, ws_down).astype(BF).astype(F32)
        s_h, s_da, s_db = act_both(sa, sb, sdh)
        ds_gate = dot_tn(x_all, s_da)
        ds_up = dot_tn(x_all, s_db)
        ds_down = dot_tn(s_h, gy_all)

        mark = slot_hit.reshape(TOK, EXPERTS * STRIP).astype(F32)
        mark16 = slot_hit[:, :, :CAP].reshape(TOK, EP, CHUNKS, PER_CHUNK, 2 * CAP).transpose(0, 1, 3, 2, 4)
        mark16 = jnp.pad(mark16, ((0, 0),) * 4 + ((0, 16 - 2 * CAP),)).reshape(TOK, EP * STEPS * 16).astype(BF)
        y_out, dx_out, d_router = finish_call(parts[0::2], firsts, o_send, x, grad_y, w_router.T, mark, mark16, all_rows)
        d_router = d_router.T
        return y_out, dx_out, d_router, d_w_gate, d_w_up, d_w_down, ds_gate, ds_up, ds_down

    tok_spec = P(('ep', 'tp'), None)
    in_specs = (tok_spec, tok_spec, P(None, None), P('ep', None, 'tp'), P('ep', None, 'tp'), P('ep', 'tp', None), P(None, 'tp'), P(None, 'tp'), P('tp', None), tok_spec)
    out_specs = (tok_spec, tok_spec, P(None, None), P('ep', None, 'tp'), P('ep', None, 'tp'), P('ep', 'tp', None), P(None, 'tp'), P(None, 'tp'), P('tp', None))
    return jax.shard_map(device_body, mesh=mesh, in_specs=in_specs, out_specs=out_specs, check_vma=False)
```
